256 devices in a mesh: member: 16 (over x, z_lo), band: 16 (over z_hi, y, core).
Axes of the slice: x: 4, y: 4, z: 8 (z_hi: 2, z_lo: 4; z = z_hi * 4 + z_lo), core: 2. Of those that a mesh axis runs over, the one named last changes fastest.
Arguments:
- prior: bfloat16 [16, 2, 768, 1536], P('member', None, 'band'), may hold values from -9 to 9
- analysis: bfloat16 [16, 2, 768, 1536], P('member', None, 'band'), may hold values from -6 to 6
- increment: float32 [2, 768, 1536], P(None, 'band'), may hold values from -6 to 6
- truncation: int32 [2], replicated, may hold values from 128 to 511
Outputs:
- members: bfloat16 [16, 2, 768, 1536], P('member', None, 'band')
The draws below stay inside these ranges and needn't reach their ends.
All inputs are finite; a program needn't handle non-finite values.
Results may differ from the reference program's by a relative error of at most 0.001.
Values sent between devices are 32-bit elements; how exact they have to be, the bound alone decides.
A program may use at most 64 MiB of HBM per device.

```python
import math
import jax
import jax.numpy as jnp
from jax import lax

NLAT = 768
NLON = 1536
MW = 512
LEV = 2
MEMBERS = 16


def block_levels(own_key, dims, split, least, top_value):
    level = 1.0
    for dim, shards_of in split:
        heights = jax.random.uniform(jax.random.fold_in(jax.random.fold_in(own_key, 6), dim), (shards_of,), jnp.float32, least / len(split), top_value / len(split))
        level = level * jnp.repeat(jnp.exp(heights), dims[dim] // shards_of).reshape((-1,) + (1,) * (len(dims) - 1 - dim))
    return level


def noise(stream_key, extent, scale, limit, split=(), kind=jnp.bfloat16):
    factor_of = block_levels(stream_key, extent, split, -0.22, 0.18) if split else 1.0
    entries = jax.random.normal(stream_key, extent, jnp.float32) * scale * factor_of
    return jnp.minimum(jnp.maximum(entries, -limit), limit).astype(kind)


def setup_inputs(seed: int = 0) -> dict:
    splits = jax.random.split(jax.random.key(seed), 5)
    return {
        "prior": noise(splits[0], (MEMBERS, LEV, NLAT, NLON), 1.5, 9.0, ((0, 16), (2, 16))),
        "analysis": noise(splits[1], (MEMBERS, LEV, NLAT, NLON), 1.0, 6.0, ((0, 16), (2, 16))),
        "increment": noise(splits[2], (LEV, NLAT, NLON), 1.0, 6.0, ((1, 16),), jnp.float32),
        "truncation": jax.random.randint(splits[3], (LEV,), MW // 4, MW).astype(jnp.int32),
    }


RELAX = 0.85
SPREAD_FLOOR = 0.25

def zonal_table(nlon, waves):
    column = jnp.arange(nlon, dtype=jnp.int32)[:, None]
    number = jnp.arange(waves, dtype=jnp.int32)[None, :]
    phase = (column * number % nlon).astype(jnp.float32) * (2.0 * math.pi / nlon)
    return jnp.stack([jnp.cos(phase), jnp.sin(phase)], axis=2).reshape(nlon, 2 * waves)

def cosine_table(nlat):
    order = jnp.arange(nlat, dtype=jnp.int32)[:, None]
    place = jnp.arange(nlat, dtype=jnp.int32)[None, :]
    phase = ((2 * place + 1) * order % (4 * nlat)).astype(jnp.float32) * (math.pi / (2.0 * nlat))
    scale = jnp.where(order == 0, jnp.float32(math.sqrt(1.0 / nlat)), jnp.float32(math.sqrt(2.0 / nlat)))
    return scale * jnp.cos(phase)

def column_weights(waves, nlon):
    number = jnp.arange(2 * waves, dtype=jnp.int32) // 2
    return jnp.where(number == 0, jnp.float32(1.0 / nlon), jnp.float32(2.0 / nlon))

def inflation(sums, count):
    mean_b = sums[0] / count
    mean_a = sums[2] / count
    spread_b = jnp.sqrt(jnp.maximum((sums[1] - count * mean_b * mean_b) / (count - 1), 0.0))
    spread_a = jnp.maximum(jnp.sqrt(jnp.maximum((sums[3] - count * mean_a * mean_a) / (count - 1), 0.0)), SPREAD_FLOOR)
    factor = 1.0 + RELAX * (spread_b - spread_a) / spread_a
    return (factor, mean_b - factor * mean_a)

def reference(prior, analysis, increment, truncation):
    count = prior.shape[0]
    b_vals = prior.astype(jnp.float32)
    a_vals = analysis.astype(jnp.float32)
    sums = jnp.stack([lax.optimization_barrier(jnp.sum(b_vals, 0)), lax.optimization_barrier(jnp.sum(b_vals * b_vals, 0)), lax.optimization_barrier(jnp.sum(a_vals, 0)), lax.optimization_barrier(jnp.sum(a_vals * a_vals, 0))])
    factor, shift = inflation(sums, count)
    levels, nlat, nlon = increment.shape
    table = zonal_table(nlon, MW)
    coef = jnp.dot(increment.reshape(levels * nlat, nlon), table, precision=lax.Precision.HIGHEST).reshape(levels, nlat, 2 * MW)
    cosines = cosine_table(nlat)
    spec = jnp.einsum('ki,lim->lkm', cosines, coef, precision=lax.Precision.HIGHEST)
    order = jnp.arange(nlat, dtype=jnp.int32)[:, None]
    number = (jnp.arange(2 * MW, dtype=jnp.int32) // 2)[None, :]
    keep = (order * order + number * number)[None] <= (truncation * truncation)[:, None, None]
    kept = jnp.einsum('ki,lkm->lim', cosines, jnp.where(keep, spec, 0.0), precision=lax.Precision.HIGHEST)
    weighted = kept * column_weights(MW, nlon)
    smooth = jnp.dot(weighted.reshape(levels * nlat, 2 * MW), table.T, precision=lax.Precision.HIGHEST).reshape(levels, nlat, nlon)
    return ((shift + smooth)[None] + factor[None] * a_vals).astype(jnp.bfloat16)
```

```python
import functools
import math

import jax
import jax.numpy as jnp
from jax import lax
from jax.experimental import pallas as pl
from jax.experimental.pallas import tpu as pltpu
from jax.sharding import PartitionSpec as P

MESH = pl.DeviceIdType.MESH
F32 = jnp.float32
BF16 = jnp.bfloat16

NX, NZ = 4, 4
BANDS, SIDE = 16, 8
LEV, ROWS, NLON = 2, 48, 1536
NLAT = BANDS * ROWS
KEEP = 512
MEMBERS = NX * NZ
QUARTER = LEV * ROWS // NX
T = 3
R = QUARTER // T
BLOCK = NLON // NZ
GROUPS = 8
WAVES = 64
COLS = 2 * WAVES

RELAX = 0.85
SPREAD_FLOOR = 0.25

COS_TERMS = [(-1.0) ** k / math.factorial(2 * k) for k in range(9)]


def cos_turn(phase, period):
    turns = jnp.floor(phase * (1.0 / period) + 0.5)
    rest = phase - turns * float(period)
    square = rest * rest * ((2.0 * math.pi / period) ** 2)
    total = jnp.full(phase.shape, COS_TERMS[-1], F32)
    for term in COS_TERMS[-2::-1]:
        total = total * square + term
    return total


def halves(values):
    high = values.astype(BF16)
    low = (values - high.astype(F32)).astype(BF16)
    return high, low


def dot(a, b):
    return jnp.dot(a, b, preferred_element_type=F32)


def dot3(a, b):
    return dot(a[0], b[0]) + (dot(a[0], b[1]) + dot(a[1], b[0]))


def iota(shape, dim):
    return lax.broadcasted_iota(jnp.int32, shape, dim)


def inflation(sums):
    count = float(MEMBERS)
    mean_b = sums[0] / count
    mean_a = sums[2] / count
    spread_b = jnp.sqrt(jnp.maximum((sums[1] - count * mean_b * mean_b) / (count - 1), 0.0))
    spread_a = jnp.maximum(
        jnp.sqrt(jnp.maximum((sums[3] - count * mean_a * mean_a) / (count - 1), 0.0)), SPREAD_FLOOR
    )
    factor = 1.0 + RELAX * (spread_b - spread_a) / spread_a
    return factor, mean_b - factor * mean_a


def kernel(
    prior_ref, analysis_ref, inc_ref, trunc_ref, out_ref,
    xs, xr, zs, zr, gr, os, orr, cf, kp, kr,
    f_hi, f_lo, c_hi, c_lo, g_hi, g_lo, sm,
    xs_s, xr_s, zs_s, zr_s, gs_s, gr_s, os_s, or_s, cs_s, cr_s, ks_s, kr_s,
):
    member = lax.axis_index("member")
    band = lax.axis_index("band")
    x, z = member // NZ, lax.rem(member, NZ)
    side, yc = band // SIDE, lax.rem(band, SIDE)
    level = x // 2
    group = lax.rem(x, 2) * NZ + z
    partner = (1 - side) * SIDE + yc

    def at_x(d):
        return lax.rem(x + d, NX)

    def at_z(d):
        return lax.rem(z + d, NZ)

    def at_band(d):
        return side * SIDE + lax.rem(yc + d, SIDE)

    def group_of(d):
        return lax.rem(group + d, GROUPS)

    def group_dev(g):
        return ((level * 2 + g // NZ) * NZ + lax.rem(g, NZ), band)

    def send(src, dst, send_sem, recv_sem, device):
        copy = pltpu.make_async_remote_copy(
            src_ref=src, dst_ref=dst, send_sem=send_sem, recv_sem=recv_sem,
            device_id=device, device_id_type=MESH,
        )
        copy.start()
        sent.append(copy)

    def arrived(dst, recv_sem):
        pltpu.make_async_remote_copy(
            src_ref=dst, dst_ref=dst, send_sem=recv_sem, recv_sem=recv_sem,
            device_id=(member, band), device_id_type=MESH,
        ).wait_recv()

    sent = []

    peers = [(at_x(d) * NZ + z, band) for d in (1, 2, 3)]
    peers += [(x * NZ + at_z(d), band) for d in (1, 2, 3)]
    other = level * 2 + (1 - lax.rem(x, 2))
    peers += [(other * NZ + at_z(d), band) for d in (1, 2, 3)]
    peers += [(member, partner)] + [(member, at_band(d)) for d in range(1, SIDE)]
    barrier = pltpu.get_barrier_semaphore()
    for peer in peers:
        pl.semaphore_signal(barrier, inc=1, device_id=peer, device_id_type=MESH)

    for lev in range(LEV):
        for field, ref in enumerate((prior_ref, analysis_ref)):
            values = ref[0, lev].astype(F32)
            for half in range(2):
                for t in range(T):
                    start = half * QUARTER + t * R
                    xs[lev * 2 + half, t, field] = values[start : start + R]

    pl.semaphore_wait(barrier, len(peers))

    for t in range(T):
        for d in (2, 1, 3):
            q = at_x(d)
            send(xs.at[q, t], xr.at[x, t], xs_s.at[t, q], xr_s.at[t, x], (q * NZ + z, band))

    def zonal_rows(n, _):
        shape = (64, COLS)
        place = (iota(shape, 0) + n * 64).astype(F32)
        lane = iota(shape, 1)
        number = (group * WAVES + lax.rem(lane, WAVES)).astype(F32)
        shifted = jnp.where(lane >= WAVES, float(NLON // 4), 0.0)
        high, low = halves(cos_turn(place * number - shifted, NLON))
        rows = pl.ds(pl.multiple_of(n * 64, 64), 64)
        f_hi[rows, :] = high
        f_lo[rows, :] = low
        return 0

    lax.fori_loop(0, NLON // 64, zonal_rows, 0)
    cf[band] = dot3(halves(inc_ref[level]), (f_hi[...], f_lo[...]))
    for d in range(1, SIDE):
        send(cf.at[band], cf.at[band], cs_s.at[d], cr_s.at[band], (member, at_band(d)))
    send(cf.at[band], cf.at[band], cs_s.at[0], cr_s.at[band], (member, partner))

    def cosine_rows(n, _):
        shape = (16, NLAT)
        order = iota(shape, 0) + n * 16
        place = (2 * iota(shape, 1) + 1).astype(F32)
        scale = jnp.where(order == 0, math.sqrt(1.0 / NLAT), math.sqrt(2.0 / NLAT))
        high, low = halves(scale * cos_turn(order.astype(F32) * place, 4 * NLAT))
        rows = pl.ds(pl.multiple_of(n * 16, 16), 16)
        c_hi[rows, :] = high
        c_lo[rows, :] = low
        return 0

    lax.fori_loop(0, KEEP // 16, cosine_rows, 0)

    arrived(cf.at[partner], cr_s.at[partner])
    for d in range(1, SIDE):
        send(
            cf.at[partner], cf.at[partner], cs_s.at[SIDE + d], cr_s.at[partner],
            (member, at_band(d)),
        )

    def sums_of(t):
        b_sum = b_sq = a_sum = a_sq = None
        for d in range(NX):
            b = xs[x, t, 0] if d == 0 else xr[at_x(d), t, 0]
            a = xs[x, t, 1] if d == 0 else xr[at_x(d), t, 1]
            if d == 0:
                b_sum, b_sq, a_sum, a_sq = b, b * b, a, a * a
            else:
                b_sum, b_sq, a_sum, a_sq = b_sum + b, b_sq + b * b, a_sum + a, a_sq + a * a
        for field, total in enumerate((b_sum, b_sq, a_sum, a_sq)):
            for block in range(NZ):
                zs[t, block, field] = total[:, block * BLOCK : (block + 1) * BLOCK]

    def spread_sums(t):
        for d in (1, 2, 3):
            arrived(xr.at[at_x(d), t], xr_s.at[t, at_x(d)])
        sums_of(t)
        for d in (2, 1, 3):
            to = at_z(d)
            send(zs.at[t, to], zr.at[t, z], zs_s.at[t, to], zr_s.at[t, z], (x * NZ + to, band))

    spread_sums(0)

    for d in range(1, SIDE):
        arrived(cf.at[at_band(d)], cr_s.at[at_band(d)])
        far = (1 - side) * SIDE + lax.rem(yc + d, SIDE)
        arrived(cf.at[far], cr_s.at[far])
    spec = dot3((c_hi[...], c_lo[...]), halves(cf[...].reshape(NLAT, COLS)))
    order = iota((KEEP, COLS), 0)
    number = group * WAVES + lax.rem(iota((KEEP, COLS), 1), WAVES)
    limit = trunc_ref[level]
    spec = jnp.where(order * order + number * number <= limit * limit, spec, 0.0)
    shape = (ROWS, KEEP)
    place = (2 * (iota(shape, 0) + band * ROWS) + 1).astype(F32)
    order = iota(shape, 1)
    scale = jnp.where(order == 0, math.sqrt(1.0 / NLAT), math.sqrt(2.0 / NLAT))
    back = halves(scale * cos_turn(order.astype(F32) * place, 4 * NLAT))
    kept = dot3(back, halves(spec))
    kp[0] = kept[:QUARTER]
    kp[1] = kept[QUARTER:]
    kr[group] = kp[group // NZ]
    for d in range(1, GROUPS):
        g = group_of(d)
        send(kp.at[g // NZ], kr.at[group], ks_s.at[d], kr_s.at[group], group_dev(g))

    spread_sums(1)

    def inverse_rows(n, _):
        shape = (32, BLOCK)
        row = iota(shape, 0) + n * 32
        number = (row // COLS) * WAVES + lax.rem(row, WAVES)
        place = (iota(shape, 1) + z * BLOCK).astype(F32)
        shifted = jnp.where(lax.rem(row, COLS) >= WAVES, float(NLON // 4), 0.0)
        weight = jnp.where(number == 0, 1.0 / NLON, 2.0 / NLON)
        high, low = halves(weight * cos_turn(place * number.astype(F32) - shifted, NLON))
        rows = pl.ds(pl.multiple_of(n * 32, 32), 32)
        g_hi[rows, :] = high
        g_lo[rows, :] = low
        return 0

    lax.fori_loop(0, GROUPS * COLS // 32, inverse_rows, 0)

    for t in range(2, T):
        spread_sums(t)

    for d in range(1, GROUPS):
        arrived(kr.at[group_of(d)], kr_s.at[group_of(d)])
    lines = jnp.concatenate([kr[g] for g in range(GROUPS)], axis=1)
    sm[...] = dot3(halves(lines), (g_hi[...], g_lo[...]))

    for t in range(T):
        for d in (1, 2, 3):
            arrived(zr.at[t, at_z(d)], zr_s.at[t, at_z(d)])
        total = zs[t, z]
        for d in (1, 2, 3):
            total = total + zr[t, at_z(d)]
        factor, shift = inflation([total[field] for field in range(4)])
        gr[t, z, 0] = factor
        gr[t, z, 1] = shift + sm[t * R : (t + 1) * R]
        for d in (2, 1, 3):
            to = at_z(d)
            send(gr.at[t, z], gr.at[t, z], gs_s.at[t, to], gr_s.at[t, z], (x * NZ + to, band))

    for t in range(T):
        for d in (1, 2, 3):
            arrived(gr.at[t, at_z(d)], gr_s.at[t, at_z(d)])
        factor = jnp.concatenate([gr[t, block, 0] for block in range(NZ)], axis=1)
        shift = jnp.concatenate([gr[t, block, 1] for block in range(NZ)], axis=1)
        for d in (2, 1, 3):
            q = at_x(d)
            os[q, t] = shift + factor * xr[q, t, 1]
            send(os.at[q, t], orr.at[x, t], os_s.at[t, q], or_s.at[t, x], (q * NZ + z, band))
        orr[x, t] = shift + factor * xs[x, t, 1]

    for t in range(T):
        for d in (1, 2, 3):
            arrived(orr.at[at_x(d), t], or_s.at[t, at_x(d)])
    for lev in range(LEV):
        out_ref[0, lev] = orr[2 * lev : 2 * lev + 2].reshape(ROWS, NLON).astype(BF16)

    for copy in sent:
        copy.wait_send()


def on_device(prior, analysis, increment, truncation):
    vmem = pl.BlockSpec(memory_space=pltpu.VMEM)
    dma = pltpu.SemaphoreType.DMA
    return pl.pallas_call(
        kernel,
        out_shape=jax.ShapeDtypeStruct((1, LEV, ROWS, NLON), BF16),
        in_specs=[vmem, vmem, vmem, pl.BlockSpec(memory_space=pltpu.SMEM)],
        out_specs=vmem,
        scratch_shapes=[
            pltpu.VMEM((NX, T, 2, R, NLON), F32),
            pltpu.VMEM((NX, T, 2, R, NLON), F32),
            pltpu.VMEM((T, NZ, 4, R, BLOCK), F32),
            pltpu.VMEM((T, NZ, 4, R, BLOCK), F32),
            pltpu.VMEM((T, NZ, 2, R, BLOCK), F32),
            pltpu.VMEM((NX, T, R, NLON), F32),
            pltpu.VMEM((NX, T, R, NLON), F32),
            pltpu.VMEM((BANDS, ROWS, COLS), F32),
            pltpu.VMEM((2, QUARTER, COLS), F32),
            pltpu.VMEM((GROUPS, QUARTER, COLS), F32),
            pltpu.VMEM((NLON, COLS), BF16),
            pltpu.VMEM((NLON, COLS), BF16),
            pltpu.VMEM((KEEP, NLAT), BF16),
            pltpu.VMEM((KEEP, NLAT), BF16),
            pltpu.VMEM((GROUPS * COLS, BLOCK), BF16),
            pltpu.VMEM((GROUPS * COLS, BLOCK), BF16),
            pltpu.VMEM((QUARTER, BLOCK), F32),
            dma((T, NX)), dma((T, NX)),
            dma((T, NZ)), dma((T, NZ)),
            dma((T, NZ)), dma((T, NZ)),
            dma((T, NX)), dma((T, NX)),
            dma((2 * SIDE,)), dma((BANDS,)),
            dma((GROUPS,)), dma((GROUPS,)),
        ],
        compiler_params=pltpu.CompilerParams(collective_id=0, has_side_effects=True),
    )(prior, analysis, increment, truncation)


def solution(mesh):
    placed = (
        P("member", None, "band", None),
        P("member", None, "band", None),
        P(None, "band", None),
        P(),
    )
    return jax.shard_map(
        on_device,
        mesh=mesh,
        in_specs=placed,
        out_specs=P("member", None, "band", None),
        check_vma=False,
    )
```

```python
import functools
import math

import jax
import jax.numpy as jnp
from jax import lax
from jax.experimental import pallas as pl
from jax.experimental.pallas import tpu as pltpu
from jax.sharding import PartitionSpec as P

MESH = pl.DeviceIdType.MESH
F32 = jnp.float32
BF16 = jnp.bfloat16

NX, NZ = 4, 4
BANDS, SIDE = 16, 8
LEV, ROWS, NLON = 2, 48, 1536
NLAT = BANDS * ROWS
KEEP = 512
MEMBERS = NX * NZ
QUARTER = LEV * ROWS // NX
R = 8
WIDTH = 512
PARTS = NLON // WIDTH
T = QUARTER // R * PARTS
PIECE = WIDTH // NZ
BLOCK = NLON // NZ
GROUPS = 8
WAVES = 64
COLS = 2 * WAVES

RELAX = 0.85
SPREAD_FLOOR = 0.25

COS_TERMS = [(-1.0) ** k / math.factorial(2 * k) for k in range(9)]


def cos_turn(phase, period):
    turns = jnp.floor(phase * (1.0 / period) + 0.5)
    rest = phase - turns * float(period)
    square = rest * rest * ((2.0 * math.pi / period) ** 2)
    total = jnp.full(phase.shape, COS_TERMS[-1], F32)
    for term in COS_TERMS[-2::-1]:
        total = total * square + term
    return total


def halves(values):
    high = values.astype(BF16)
    low = (values - high.astype(F32)).astype(BF16)
    return high, low


def dot(a, b):
    return jnp.dot(a, b, preferred_element_type=F32)


def dot3(a, b):
    return dot(a[0], b[0]) + (dot(a[0], b[1]) + dot(a[1], b[0]))


def iota(shape, dim):
    return lax.broadcasted_iota(jnp.int32, shape, dim)


def inflation(sums):
    count = float(MEMBERS)
    mean_b = sums[0] / count
    mean_a = sums[2] / count
    spread_b = jnp.sqrt(jnp.maximum((sums[1] - count * mean_b * mean_b) / (count - 1), 0.0))
    spread_a = jnp.maximum(
        jnp.sqrt(jnp.maximum((sums[3] - count * mean_a * mean_a) / (count - 1), 0.0)), SPREAD_FLOOR
    )
    factor = 1.0 + RELAX * (spread_b - spread_a) / spread_a
    return factor, mean_b - factor * mean_a


def kernel(
    prior_ref, analysis_ref, inc_ref, trunc_ref, out_ref,
    prior, analysis, inc, trunc, xs, xr, zs, zr, zc, gr, os, cf, kp, kr,
    f_hi, f_lo, c_hi, c_lo, g_hi, g_lo, sm,
    xs_s, xr_s, zs_s, zr_s, gs_s, gr_s, os_s, or_s, cs_s, cr_s, ks_s, kr_s, in_s, reach,
):
    member = lax.axis_index("member")
    band = lax.axis_index("band")
    x, z = member // NZ, lax.rem(member, NZ)
    side, yc = band // SIDE, lax.rem(band, SIDE)
    level = x // 2
    group = lax.rem(x, 2) * NZ + z
    partner = (1 - side) * SIDE + yc
    line = side * NZ + z

    def at_x(d):
        return lax.rem(x + d, NX)

    def at_z(d):
        return lax.rem(z + d, NZ)

    def at_band(d):
        return side * SIDE + lax.rem(yc + d, SIDE)

    def group_of(d):
        return lax.rem(group + d, GROUPS)

    def group_dev(g):
        return ((level * 2 + g // NZ) * NZ + lax.rem(g, NZ), band)

    def on_line(place):
        return (x * NZ + lax.rem(place, NZ), place // NZ * SIDE + yc)

    def send(src, dst, send_sem, recv_sem, device):
        copy = pltpu.make_async_remote_copy(
            src_ref=src, dst_ref=dst, send_sem=send_sem, recv_sem=recv_sem,
            device_id=device, device_id_type=MESH,
        )
        copy.start()
        return copy

    def left(src, send_sem):
        pltpu.make_async_remote_copy(
            src_ref=src, dst_ref=src, send_sem=send_sem, recv_sem=send_sem,
            device_id=(member, band), device_id_type=MESH,
        ).wait_send()

    def arrived(dst, recv_sem):
        pltpu.make_async_remote_copy(
            src_ref=dst, dst_ref=dst, send_sem=recv_sem, recv_sem=recv_sem,
            device_id=(member, band), device_id_type=MESH,
        ).wait_recv()

    loads = [
        pltpu.make_async_copy(prior_ref.at[0], prior, in_s.at[0]),
        pltpu.make_async_copy(analysis_ref.at[0], analysis, in_s.at[1]),
        pltpu.make_async_copy(inc_ref.at[level], inc, in_s.at[2]),
        pltpu.make_async_copy(trunc_ref, trunc, in_s.at[3]),
    ]
    for load in loads:
        load.start()

    peers = [(at_x(d) * NZ + z, band) for d in (1, 2, 3)]
    peers += [(member, at_band(d)) for d in range(1, SIDE)]
    barrier = pltpu.get_barrier_semaphore()

    def tell_line(semaphore):
        @pl.when(line > 0)
        def _():
            pl.semaphore_signal(
                semaphore, inc=1, device_id=on_line(line - 1), device_id_type=MESH
            )

        @pl.when(line < 2 * NZ - 1)
        def _():
            pl.semaphore_signal(
                semaphore, inc=1, device_id=on_line(line + 1), device_id_type=MESH
            )

    beside = (line > 0).astype(jnp.int32) + (line < 2 * NZ - 1).astype(jnp.int32)
    for peer in peers:
        pl.semaphore_signal(barrier, inc=1, device_id=peer, device_id_type=MESH)
    tell_line(barrier)

    def tell(stage):
        tell_line(reach.at[stage])

    def told(stage):
        pl.semaphore_wait(reach.at[stage], beside)

    def zonal_rows(n, _):
        shape = (64, COLS)
        place = (iota(shape, 0) + n * 64).astype(F32)
        lane = iota(shape, 1)
        number = (group * WAVES + lax.rem(lane, WAVES)).astype(F32)
        shifted = jnp.where(lane >= WAVES, float(NLON // 4), 0.0)
        high, low = halves(cos_turn(place * number - shifted, NLON))
        rows = pl.ds(pl.multiple_of(n * 64, 64), 64)
        f_hi[rows, :] = high
        f_lo[rows, :] = low
        return 0

    def cosine_rows(n, _):
        shape = (16, NLAT)
        order = iota(shape, 0) + n * 16
        place = (2 * iota(shape, 1) + 1).astype(F32)
        scale = jnp.where(order == 0, math.sqrt(1.0 / NLAT), math.sqrt(2.0 / NLAT))
        high, low = halves(scale * cos_turn(order.astype(F32) * place, 4 * NLAT))
        rows = pl.ds(pl.multiple_of(n * 16, 16), 16)
        c_hi[rows, :] = high
        c_lo[rows, :] = low
        return 0

    def inverse_rows(n, _):
        shape = (32, BLOCK)
        row = iota(shape, 0) + n * 32
        number = (row // COLS) * WAVES + lax.rem(row, WAVES)
        lane = iota(shape, 1)
        place = (lane // PIECE * WIDTH + z * PIECE + lax.rem(lane, PIECE)).astype(F32)
        shifted = jnp.where(lax.rem(row, COLS) >= WAVES, float(NLON // 4), 0.0)
        weight = jnp.where(number == 0, 1.0 / NLON, 2.0 / NLON)
        high, low = halves(weight * cos_turn(place * number.astype(F32) - shifted, NLON))
        rows = pl.ds(pl.multiple_of(n * 32, 32), 32)
        g_hi[rows, :] = high
        g_lo[rows, :] = low
        return 0

    cosine_steps = KEEP // 16
    inverse_steps = GROUPS * COLS // 32

    end = (z == 0) | (z == NZ - 1)
    middle = jnp.logical_not(end)
    start = jnp.where(z < 2, 1, 0)
    beyond = jnp.where(z < 2, 1 - z, 5 - z)
    across = 3 - z
    far_end = jnp.where(z == 1, 3, 0)
    other_middle = 3 - z

    def spread_sums(t):
        for d in (1, 3, 2):
            arrived(xr.at[at_x(d), t], xr_s.at[t, at_x(d)])
        b_sum = b_sq = a_sum = a_sq = None
        for d in range(NX):
            b = xs[x, t, 0] if d == 0 else xr[at_x(d), t, 0]
            a = xs[x, t, 1] if d == 0 else xr[at_x(d), t, 1]
            if d == 0:
                b_sum, b_sq, a_sum, a_sq = b, b * b, a, a * a
            else:
                b_sum, b_sq, a_sum, a_sq = b_sum + b, b_sq + b * b, a_sum + a, a_sq + a * a
        for field, total in enumerate((b_sum, b_sq, a_sum, a_sq)):
            for block in range(NZ):
                zs[t, block, field] = total[:, block * PIECE : (block + 1) * PIECE]

        @pl.when(end)
        def _():
            send(
                zs.at[t, pl.ds(start, 3)], zr.at[t, pl.ds(0, 3)], zs_s.at[t, 0], zr_s.at[t, 0],
                (x * NZ + beyond, band),
            )

        @pl.when(middle)
        def _():
            send(
                zs.at[t, beyond], zr.at[t, 0], zs_s.at[t, 0], zr_s.at[t, 0],
                (x * NZ + beyond, band),
            )

    def pass_on(t):
        @pl.when(middle)
        def _():
            arrived(zr.at[t, pl.ds(0, 3)], zr_s.at[t, 0])
            for k, to in enumerate((far_end, other_middle)):
                zc[t, k] = zs[t, to] + zr[t, to - start]
                send(
                    zc.at[t, k], zr.at[t, 3], zs_s.at[t, 1 + k], zr_s.at[t, 1],
                    (x * NZ + to, band),
                )

    def spread_factors(t):
        @pl.when(end)
        def _():
            arrived(zr.at[t, 0], zr_s.at[t, 0])

        arrived(zr.at[t, 3], zr_s.at[t, 1])
        total = zs[t, z] + zr[t, jnp.where(z == 2, 2, 0)] + zr[t, 3]
        factor, shift = inflation([total[field] for field in range(4)])
        gr[t, z, 0] = factor
        gr[t, z, 1] = shift + sm[
            t // PARTS * R : t // PARTS * R + R, t % PARTS * PIECE : (t % PARTS + 1) * PIECE
        ]
        for d in (2, 1, 3):
            to = at_z(d)
            send(gr.at[t, z], gr.at[t, z], gs_s.at[t, to], gr_s.at[t, z], (x * NZ + to, band))

    top = lax.rem(x, 2) * QUARTER

    def update(t):
        for d in (1, 2, 3):
            arrived(gr.at[t, at_z(d)], gr_s.at[t, at_z(d)])
        factor = jnp.concatenate([gr[t, block, 0] for block in range(NZ)], axis=1)
        shift = jnp.concatenate([gr[t, block, 1] for block in range(NZ)], axis=1)
        rows = pl.ds(pl.multiple_of(top + t // PARTS * R, R), R)
        lanes = pl.ds(t % PARTS * WIDTH, WIDTH)
        for d in (2, 1, 3):
            q = at_x(d)
            os[q, t] = shift + factor * xr[q, t, 1]
            send(
                os.at[q, t], out_ref.at[0, level, rows, lanes], os_s.at[t, q], or_s.at[t, x],
                (q * NZ + z, band),
            )
        out_ref[0, level, rows, lanes] = shift + factor * xs[x, t, 1]

    lax.fori_loop(0, NLON // 64, zonal_rows, 0)
    loads[0].wait()
    loads[1].wait()
    for lev in range(LEV):
        for field, ref in enumerate((prior, analysis)):
            values = ref[lev].astype(F32)
            for half in range(2):
                for t in range(T):
                    r = half * QUARTER + t // PARTS * R
                    w = t % PARTS * WIDTH
                    xs[lev * 2 + half, t, field] = values[r : r + R, w : w + WIDTH]

    pl.semaphore_wait(barrier, len(peers) + beside)
    tell(0)
    for t in range(T):
        for d in (2, 1, 3):
            q = at_x(d)
            send(xs.at[q, t], xr.at[x, t], xs_s.at[t, q], xr_s.at[t, x], (q * NZ + z, band))

    loads[2].wait()
    loads[3].wait()
    cf[band] = dot3(halves(inc[...]), (f_hi[...], f_lo[...]))
    for d in range(1, SIDE):
        send(cf.at[band], cf.at[band], cs_s.at[d], cr_s.at[band], (member, at_band(d)))
    told(0)
    tell(1)
    lax.fori_loop(0, cosine_steps // 4, cosine_rows, 0)
    told(1)
    tell(2)
    lax.fori_loop(cosine_steps // 4, cosine_steps // 2, cosine_rows, 0)
    told(2)
    send(cf.at[band], cf.at[band], cs_s.at[0], cr_s.at[band], (member, partner))
    spread_sums(0)
    lax.fori_loop(cosine_steps // 2, cosine_steps, cosine_rows, 0)
    spread_sums(1)
    spread_sums(2)
    pass_on(0)
    spread_sums(3)
    pass_on(1)
    arrived(cf.at[partner], cr_s.at[partner])
    for d in range(1, SIDE):
        send(
            cf.at[partner], cf.at[partner], cs_s.at[SIDE + d], cr_s.at[partner],
            (member, at_band(d)),
        )
    lax.fori_loop(0, inverse_steps // 2, inverse_rows, 0)
    spread_sums(4)
    pass_on(2)
    lax.fori_loop(inverse_steps // 2, inverse_steps, inverse_rows, 0)
    spread_sums(5)
    pass_on(3)

    for d in range(1, SIDE):
        arrived(cf.at[at_band(d)], cr_s.at[at_band(d)])
        far = (1 - side) * SIDE + lax.rem(yc + d, SIDE)
        arrived(cf.at[far], cr_s.at[far])
    spec = dot3((c_hi[...], c_lo[...]), halves(cf[...].reshape(NLAT, COLS)))
    order = iota((KEEP, COLS), 0)
    number = group * WAVES + lax.rem(iota((KEEP, COLS), 1), WAVES)
    limit = trunc[level]
    spec = jnp.where(order * order + number * number <= limit * limit, spec, 0.0)
    shape = (ROWS, KEEP)
    place = (2 * (iota(shape, 0) + band * ROWS) + 1).astype(F32)
    order = iota(shape, 1)
    scale = jnp.where(order == 0, math.sqrt(1.0 / NLAT), math.sqrt(2.0 / NLAT))
    back = halves(scale * cos_turn(order.astype(F32) * place, 4 * NLAT))
    kept = dot3(back, halves(spec))
    kp[0] = kept[:QUARTER]
    kp[1] = kept[QUARTER:]
    kr[group] = kp[group // NZ]
    for d in range(1, GROUPS):
        g = group_of(d)
        send(kp.at[g // NZ], kr.at[group], ks_s.at[d], kr_s.at[group], group_dev(g))

    for t in range(6, T):
        spread_sums(t)
        pass_on(t - 2)
    pass_on(T - 2)
    pass_on(T - 1)

    for d in range(1, GROUPS):
        arrived(kr.at[group_of(d)], kr_s.at[group_of(d)])
    lines = jnp.concatenate([kr[g] for g in range(GROUPS)], axis=1)
    sm[...] = dot3(halves(lines), (g_hi[...], g_lo[...]))

    for t in range(T):
        spread_factors(t)
    for t in range(T):
        update(t)

    for t in range(T):
        for d in (1, 2, 3):
            q = at_x(d)
            rows = pl.ds(pl.multiple_of(lax.rem(q, 2) * QUARTER + t // PARTS * R, R), R)
            arrived(
                out_ref.at[0, q // 2, rows, pl.ds(t % PARTS * WIDTH, WIDTH)], or_s.at[t, q]
            )

    for t in range(T):
        for d in (1, 2, 3):
            left(xs.at[at_x(d), t], xs_s.at[t, at_x(d)])
            left(gr.at[t, z], gs_s.at[t, at_z(d)])
            left(os.at[at_x(d), t], os_s.at[t, at_x(d)])
    for d in range(1, SIDE):
        left(cf.at[band], cs_s.at[d])
        left(cf.at[partner], cs_s.at[SIDE + d])
        left(kp.at[group_of(d) // NZ], ks_s.at[d])
    left(cf.at[band], cs_s.at[0])

    @pl.when(end)
    def _():
        for t in range(T):
            left(zs.at[t, pl.ds(start, 3)], zs_s.at[t, 0])

    @pl.when(middle)
    def _():
        for t in range(T):
            left(zs.at[t, beyond], zs_s.at[t, 0])
            left(zc.at[t, 0], zs_s.at[t, 1])
            left(zc.at[t, 1], zs_s.at[t, 2])


def on_device(prior, analysis, increment, truncation):
    vmem = pl.BlockSpec(memory_space=pltpu.VMEM)
    hbm = pl.BlockSpec(memory_space=pltpu.HBM)
    dma = pltpu.SemaphoreType.DMA
    return pl.pallas_call(
        kernel,
        out_shape=pltpu.VMEM((1, LEV, ROWS, NLON), F32),
        in_specs=[hbm, hbm, hbm, hbm],
        out_specs=vmem,
        scratch_shapes=[
            pltpu.VMEM((LEV, ROWS, NLON), BF16),
            pltpu.VMEM((LEV, ROWS, NLON), BF16),
            pltpu.VMEM((ROWS, NLON), F32),
            pltpu.SMEM((LEV,), jnp.int32),
            pltpu.VMEM((NX, T, 2, R, WIDTH), F32),
            pltpu.VMEM((NX, T, 2, R, WIDTH), F32),
            pltpu.VMEM((T, NZ, 4, R, PIECE), F32),
            pltpu.VMEM((T, NZ, 4, R, PIECE), F32),
            pltpu.VMEM((T, 2, 4, R, PIECE), F32),
            pltpu.VMEM((T, NZ, 2, R, PIECE), F32),
            pltpu.VMEM((NX, T, R, WIDTH), F32),
            pltpu.VMEM((BANDS, ROWS, COLS), F32),
            pltpu.VMEM((2, QUARTER, COLS), F32),
            pltpu.VMEM((GROUPS, QUARTER, COLS), F32),
            pltpu.VMEM((NLON, COLS), BF16),
            pltpu.VMEM((NLON, COLS), BF16),
            pltpu.VMEM((KEEP, NLAT), BF16),
            pltpu.VMEM((KEEP, NLAT), BF16),
            pltpu.VMEM((GROUPS * COLS, BLOCK), BF16),
            pltpu.VMEM((GROUPS * COLS, BLOCK), BF16),
            pltpu.VMEM((QUARTER, BLOCK), F32),
            dma((T, NX)), dma((T, NX)),
            dma((T, NZ)), dma((T, NZ)),
            dma((T, NZ)), dma((T, NZ)),
            dma((T, NX)), dma((T, NX)),
            dma((2 * SIDE,)), dma((BANDS,)),
            dma((GROUPS,)), dma((GROUPS,)),
            dma((4,)), pltpu.SemaphoreType.REGULAR((3,)),
        ],
        compiler_params=pltpu.CompilerParams(collective_id=0, has_side_effects=True),
    )(prior, analysis, increment, truncation).astype(BF16)


def solution(mesh):
    placed = (
        P("member", None, "band", None),
        P("member", None, "band", None),
        P(None, "band", None),
        P(),
    )
    return jax.shard_map(
        on_device,
        mesh=mesh,
        in_specs=placed,
        out_specs=P("member", None, "band", None),
        check_vma=False,
    )
```

```python
import functools
import math

import jax
import jax.numpy as jnp
from jax import lax
from jax.experimental import pallas as pl
from jax.experimental.pallas import tpu as pltpu
from jax.sharding import PartitionSpec as P

MESH = pl.DeviceIdType.MESH
F32 = jnp.float32
BF16 = jnp.bfloat16

NX, NZ = 4, 4
BANDS, SIDE = 16, 8
LEV, ROWS, NLON = 2, 48, 1536
NLAT = BANDS * ROWS
KEEP = 512
MEMBERS = NX * NZ
QUARTER = LEV * ROWS // NX
R = 8
WIDTH = 512
PARTS = NLON // WIDTH
T = QUARTER // R * PARTS
PIECE = WIDTH // NZ
BLOCK = NLON // NZ
GROUPS = 8
WAVES = 64
COLS = 2 * WAVES

RELAX = 0.85
SPREAD_FLOOR = 0.25

COS_TERMS = [(-1.0) ** k / math.factorial(2 * k) for k in range(9)]


def cos_turn(phase, period):
    turns = jnp.floor(phase * (1.0 / period) + 0.5)
    rest = phase - turns * float(period)
    square = rest * rest * ((2.0 * math.pi / period) ** 2)
    total = jnp.full(phase.shape, COS_TERMS[-1], F32)
    for term in COS_TERMS[-2::-1]:
        total = total * square + term
    return total


def halves(values):
    high = values.astype(BF16)
    low = (values - high.astype(F32)).astype(BF16)
    return high, low


def dot(a, b):
    return jnp.dot(a, b, preferred_element_type=F32)


def dot3(a, b):
    return dot(a[0], b[0]) + (dot(a[0], b[1]) + dot(a[1], b[0]))


def iota(shape, dim):
    return lax.broadcasted_iota(jnp.int32, shape, dim)


def inflation(sums):
    count = float(MEMBERS)
    mean_b = sums[0] / count
    mean_a = sums[2] / count
    spread_b = jnp.sqrt(jnp.maximum((sums[1] - count * mean_b * mean_b) / (count - 1), 0.0))
    spread_a = jnp.maximum(
        jnp.sqrt(jnp.maximum((sums[3] - count * mean_a * mean_a) / (count - 1), 0.0)), SPREAD_FLOOR
    )
    factor = 1.0 + RELAX * (spread_b - spread_a) / spread_a
    return factor, mean_b - factor * mean_a


def kernel(
    prior_ref, analysis_ref, inc_ref, trunc_ref, out_ref,
    prior, analysis, inc, trunc, xs, xr, zs, zr, zc, gr, os, cf, ps, pr, kp, kr,
    f_hi, f_lo, c_hi, c_lo, g_hi, g_lo, sm,
    xs_s, xr_s, zs_s, zr_s, gs_s, gr_s, os_s, or_s, cs_s, cr_s, ks_s, kr_s, in_s, reach,
):
    member = lax.axis_index("member")
    band = lax.axis_index("band")
    x, z = member // NZ, lax.rem(member, NZ)
    side, yc = band // SIDE, lax.rem(band, SIDE)
    level = x // 2
    group = lax.rem(x, 2) * NZ + z
    partner = (1 - side) * SIDE + yc
    mate = (level * 2 + 1 - lax.rem(x, 2)) * NZ + z

    def at_x(d):
        return lax.rem(x + d, NX)

    def at_z(d):
        return lax.rem(z + d, NZ)

    def at_band(d):
        return side * SIDE + lax.rem(yc + d, SIDE)

    def group_of(d):
        return lax.rem(group + d, GROUPS)

    def group_dev(g):
        return ((level * 2 + g // NZ) * NZ + lax.rem(g, NZ), band)

    def send(src, dst, send_sem, recv_sem, device):
        copy = pltpu.make_async_remote_copy(
            src_ref=src, dst_ref=dst, send_sem=send_sem, recv_sem=recv_sem,
            device_id=device, device_id_type=MESH,
        )
        copy.start()
        return copy

    def left(src, send_sem):
        pltpu.make_async_remote_copy(
            src_ref=src, dst_ref=src, send_sem=send_sem, recv_sem=send_sem,
            device_id=(member, band), device_id_type=MESH,
        ).wait_send()

    def arrived(dst, recv_sem):
        pltpu.make_async_remote_copy(
            src_ref=dst, dst_ref=dst, send_sem=recv_sem, recv_sem=recv_sem,
            device_id=(member, band), device_id_type=MESH,
        ).wait_recv()

    loads = [
        pltpu.make_async_copy(prior_ref.at[0], prior, in_s.at[0]),
        pltpu.make_async_copy(analysis_ref.at[0], analysis, in_s.at[1]),
        pltpu.make_async_copy(inc_ref.at[level], inc, in_s.at[2]),
        pltpu.make_async_copy(trunc_ref, trunc, in_s.at[3]),
    ]
    for load in loads:
        load.start()

    peers = [(at_x(d) * NZ + z, band) for d in (1, 2, 3)]
    peers += [(member, at_band(d)) for d in range(1, SIDE)]
    barrier = pltpu.get_barrier_semaphore()

    near = ((z > 0, member - 1), (z < NZ - 1, member + 1))
    neighbours = (z > 0).astype(jnp.int32) + (z < NZ - 1).astype(jnp.int32)

    def tell(semaphore):
        for there, device in near:

            @pl.when(there)
            def _():
                pl.semaphore_signal(
                    semaphore, inc=1, device_id=(device, band), device_id_type=MESH
                )

    for peer in peers:
        pl.semaphore_signal(barrier, inc=1, device_id=peer, device_id_type=MESH)
    tell(barrier)

    @pl.when(side == 0)
    def _():
        pl.semaphore_signal(barrier, inc=1, device_id=(member, partner), device_id_type=MESH)

    def zonal_rows(n, _):
        shape = (64, COLS)
        place = (iota(shape, 0) + n * 64).astype(F32)
        lane = iota(shape, 1)
        number = (group * WAVES + lax.rem(lane, WAVES)).astype(F32)
        shifted = jnp.where(lane >= WAVES, float(NLON // 4), 0.0)
        high, low = halves(cos_turn(place * number - shifted, NLON))
        rows = pl.ds(pl.multiple_of(n * 64, 64), 64)
        f_hi[rows, :] = high
        f_lo[rows, :] = low
        return 0

    def cosine_rows(n, _):
        shape = (16, SIDE * ROWS)
        order = iota(shape, 0) + n * 16
        place = (2 * (iota(shape, 1) + side * SIDE * ROWS) + 1).astype(F32)
        scale = jnp.where(order == 0, math.sqrt(1.0 / NLAT), math.sqrt(2.0 / NLAT))
        high, low = halves(scale * cos_turn(order.astype(F32) * place, 4 * NLAT))
        rows = pl.ds(pl.multiple_of(n * 16, 16), 16)
        c_hi[rows, :] = high
        c_lo[rows, :] = low
        return 0

    def inverse_rows(n, _):
        shape = (32, BLOCK)
        row = iota(shape, 0) + n * 32
        number = (row // COLS) * WAVES + lax.rem(row, WAVES)
        lane = iota(shape, 1)
        place = (lane // PIECE * WIDTH + z * PIECE + lax.rem(lane, PIECE)).astype(F32)
        shifted = jnp.where(lax.rem(row, COLS) >= WAVES, float(NLON // 4), 0.0)
        weight = jnp.where(number == 0, 1.0 / NLON, 2.0 / NLON)
        high, low = halves(weight * cos_turn(place * number.astype(F32) - shifted, NLON))
        rows = pl.ds(pl.multiple_of(n * 32, 32), 32)
        g_hi[rows, :] = high
        g_lo[rows, :] = low
        return 0

    cosine_steps = KEEP // 16
    inverse_steps = GROUPS * COLS // 32

    end = (z == 0) | (z == NZ - 1)
    middle = jnp.logical_not(end)
    start = jnp.where(z < 2, 1, 0)
    beyond = jnp.where(z < 2, 1 - z, 5 - z)
    across = 3 - z
    far_end = jnp.where(z == 1, 3, 0)
    other_middle = 3 - z

    def spread_sums(t):
        for d in (1, 3, 2):
            arrived(xr.at[at_x(d), t], xr_s.at[t, at_x(d)])
        b_sum = b_sq = a_sum = a_sq = None
        for d in range(NX):
            b = xs[x, t, 0] if d == 0 else xr[at_x(d), t, 0]
            a = xs[x, t, 1] if d == 0 else xr[at_x(d), t, 1]
            if d == 0:
                b_sum, b_sq, a_sum, a_sq = b, b * b, a, a * a
            else:
                b_sum, b_sq, a_sum, a_sq = b_sum + b, b_sq + b * b, a_sum + a, a_sq + a * a
        for field, total in enumerate((b_sum, b_sq, a_sum, a_sq)):
            for block in range(NZ):
                zs[t, block, field] = total[:, block * PIECE : (block + 1) * PIECE]

        @pl.when(end)
        def _():
            send(
                zs.at[t, pl.ds(start, 3)], zr.at[t, pl.ds(0, 3)], zs_s.at[t, 0], zr_s.at[t, 0],
                (x * NZ + beyond, band),
            )

        @pl.when(middle)
        def _():
            send(
                zs.at[t, beyond], zr.at[t, 0], zs_s.at[t, 0], zr_s.at[t, 0],
                (x * NZ + beyond, band),
            )

    def pass_on(t):
        @pl.when(middle)
        def _():
            arrived(zr.at[t, pl.ds(0, 3)], zr_s.at[t, 0])
            for k, to in enumerate((far_end, other_middle)):
                zc[t, k] = zs[t, to] + zr[t, to - start]
                send(
                    zc.at[t, k], zr.at[t, 3], zs_s.at[t, 1 + k], zr_s.at[t, 1],
                    (x * NZ + to, band),
                )

    def spread_factors(t):
        @pl.when(end)
        def _():
            arrived(zr.at[t, 0], zr_s.at[t, 0])

        arrived(zr.at[t, 3], zr_s.at[t, 1])
        total = zs[t, z] + zr[t, jnp.where(z == 2, 2, 0)] + zr[t, 3]
        factor, shift = inflation([total[field] for field in range(4)])
        gr[t, z, 0] = factor
        gr[t, z, 1] = shift + sm[
            t // PARTS * R : t // PARTS * R + R, t % PARTS * PIECE : (t % PARTS + 1) * PIECE
        ]
        for d in (2, 1, 3):
            to = at_z(d)
            send(gr.at[t, z], gr.at[t, z], gs_s.at[t, to], gr_s.at[t, z], (x * NZ + to, band))

    top = lax.rem(x, 2) * QUARTER

    def update(t):
        for d in (1, 2, 3):
            arrived(gr.at[t, at_z(d)], gr_s.at[t, at_z(d)])
        factor = jnp.concatenate([gr[t, block, 0] for block in range(NZ)], axis=1)
        shift = jnp.concatenate([gr[t, block, 1] for block in range(NZ)], axis=1)
        rows = pl.ds(pl.multiple_of(top + t // PARTS * R, R), R)
        lanes = pl.ds(t % PARTS * WIDTH, WIDTH)
        for d in (2, 1, 3):
            q = at_x(d)
            os[q, t] = shift + factor * xr[q, t, 1]
            send(
                os.at[q, t], out_ref.at[0, level, rows, lanes], os_s.at[t, q], or_s.at[t, x],
                (q * NZ + z, band),
            )
        out_ref[0, level, rows, lanes] = shift + factor * xs[x, t, 1]

    lax.fori_loop(0, NLON // 64, zonal_rows, 0)
    loads[0].wait()
    loads[1].wait()
    for lev in range(LEV):
        for field, ref in enumerate((prior, analysis)):
            values = ref[lev].astype(F32)
            for half in range(2):
                for t in range(T):
                    r = half * QUARTER + t // PARTS * R
                    w = t % PARTS * WIDTH
                    xs[lev * 2 + half, t, field] = values[r : r + R, w : w + WIDTH]

    pl.semaphore_wait(barrier, len(peers) + neighbours + side)
    for t in range(T):
        for d in (2, 1, 3):
            q = at_x(d)
            send(xs.at[q, t], xr.at[x, t], xs_s.at[t, q], xr_s.at[t, x], (q * NZ + z, band))
    tell(reach.at[0])

    @pl.when(side == 1)
    def _():
        pl.semaphore_signal(reach.at[3], inc=1, device_id=(member, partner), device_id_type=MESH)


    loads[2].wait()
    loads[3].wait()
    cf[yc] = dot3(halves(inc[...]), (f_hi[...], f_lo[...]))
    for d in range(1, SIDE):
        send(cf.at[yc], cf.at[yc], cs_s.at[d], cr_s.at[yc], (member, at_band(d)))
    lax.fori_loop(0, cosine_steps, cosine_rows, 0)
    lax.fori_loop(0, inverse_steps // 2, inverse_rows, 0)
    pl.semaphore_wait(reach.at[0], neighbours)
    tell(reach.at[1])
    lax.fori_loop(inverse_steps // 2, inverse_steps, inverse_rows, 0)

    for d in range(1, SIDE):
        other = lax.rem(yc + d, SIDE)
        arrived(cf.at[other], cr_s.at[other])
    spec = dot3((c_hi[...], c_lo[...]), halves(cf[...].reshape(SIDE * ROWS, COLS)))
    order = iota((KEEP, COLS), 0)
    number = group * WAVES + lax.rem(iota((KEEP, COLS), 1), WAVES)
    limit = trunc[level]
    spec = jnp.where(order * order + number * number <= limit * limit, spec, 0.0)
    shape = (2 * ROWS, KEEP)
    row = iota(shape, 0)
    place = row + jnp.where(row < ROWS, band, partner - 1) * ROWS
    order = iota(shape, 1)
    scale = jnp.where(order == 0, math.sqrt(1.0 / NLAT), math.sqrt(2.0 / NLAT))
    back = scale * cos_turn(order.astype(F32) * (2 * place + 1).astype(F32), 4 * NLAT)
    parts = dot3(halves(back), halves(spec))
    ps[0] = parts[:ROWS]
    ps[1] = parts[ROWS:]

    @pl.when(side == 0)
    def _():
        pl.semaphore_wait(reach.at[3], 1)

    send(ps.at[1], pr, cs_s.at[0], cr_s.at[SIDE], (member, partner))
    spread_sums(0)
    pl.semaphore_wait(reach.at[1], neighbours)
    pl.semaphore_signal(reach.at[2], inc=1, device_id=(mate, band), device_id_type=MESH)
    spread_sums(1)
    spread_sums(2)
    pass_on(0)
    spread_sums(3)
    pass_on(1)
    spread_sums(4)
    pass_on(2)
    pl.semaphore_wait(reach.at[2], 1)
    arrived(pr, cr_s.at[SIDE])
    for half in range(2):
        kp[half] = ps[0, half * QUARTER : (half + 1) * QUARTER] + pr[half * QUARTER : (half + 1) * QUARTER]
    kr[group] = kp[group // NZ]
    for d in range(1, GROUPS):
        g = group_of(d)
        send(kp.at[g // NZ], kr.at[group], ks_s.at[d], kr_s.at[group], group_dev(g))
    for t in range(5, T):
        spread_sums(t)
        pass_on(t - 2)

    for d in range(1, GROUPS):
        arrived(kr.at[group_of(d)], kr_s.at[group_of(d)])
    lines = jnp.concatenate([kr[g] for g in range(GROUPS)], axis=1)
    sm[...] = dot3(halves(lines), (g_hi[...], g_lo[...]))

    for t in range(4):
        spread_factors(t)
    pass_on(7)
    spread_factors(4)
    spread_factors(5)
    pass_on(8)
    spread_factors(6)
    update(0)
    spread_factors(7)
    update(1)
    update(2)
    spread_factors(8)
    for t in range(3, T):
        update(t)

    for t in range(T):
        for d in (1, 2, 3):
            q = at_x(d)
            rows = pl.ds(pl.multiple_of(lax.rem(q, 2) * QUARTER + t // PARTS * R, R), R)
            arrived(
                out_ref.at[0, q // 2, rows, pl.ds(t % PARTS * WIDTH, WIDTH)], or_s.at[t, q]
            )

    for t in range(T):
        for d in (1, 2, 3):
            left(xs.at[at_x(d), t], xs_s.at[t, at_x(d)])
            left(gr.at[t, z], gs_s.at[t, at_z(d)])
            left(os.at[at_x(d), t], os_s.at[t, at_x(d)])
    for d in range(1, SIDE):
        left(cf.at[yc], cs_s.at[d])
        left(kp.at[group_of(d) // NZ], ks_s.at[d])
    left(ps.at[1], cs_s.at[0])

    @pl.when(end)
    def _():
        for t in range(T):
            left(zs.at[t, pl.ds(start, 3)], zs_s.at[t, 0])

    @pl.when(middle)
    def _():
        for t in range(T):
            left(zs.at[t, beyond], zs_s.at[t, 0])
            left(zc.at[t, 0], zs_s.at[t, 1])
            left(zc.at[t, 1], zs_s.at[t, 2])


def on_device(prior, analysis, increment, truncation):
    vmem = pl.BlockSpec(memory_space=pltpu.VMEM)
    hbm = pl.BlockSpec(memory_space=pltpu.HBM)
    dma = pltpu.SemaphoreType.DMA
    return pl.pallas_call(
        kernel,
        out_shape=pltpu.VMEM((1, LEV, ROWS, NLON), F32),
        in_specs=[hbm, hbm, hbm, hbm],
        out_specs=vmem,
        scratch_shapes=[
            pltpu.VMEM((LEV, ROWS, NLON), BF16),
            pltpu.VMEM((LEV, ROWS, NLON), BF16),
            pltpu.VMEM((ROWS, NLON), F32),
            pltpu.SMEM((LEV,), jnp.int32),
            pltpu.VMEM((NX, T, 2, R, WIDTH), F32),
            pltpu.VMEM((NX, T, 2, R, WIDTH), F32),
            pltpu.VMEM((T, NZ, 4, R, PIECE), F32),
            pltpu.VMEM((T, NZ, 4, R, PIECE), F32),
            pltpu.VMEM((T, 2, 4, R, PIECE), F32),
            pltpu.VMEM((T, NZ, 2, R, PIECE), F32),
            pltpu.VMEM((NX, T, R, WIDTH), F32),
            pltpu.VMEM((SIDE, ROWS, COLS), F32),
            pltpu.VMEM((2, ROWS, COLS), F32),
            pltpu.VMEM((ROWS, COLS), F32),
            pltpu.VMEM((2, QUARTER, COLS), F32),
            pltpu.VMEM((GROUPS, QUARTER, COLS), F32),
            pltpu.VMEM((NLON, COLS), BF16),
            pltpu.VMEM((NLON, COLS), BF16),
            pltpu.VMEM((KEEP, SIDE * ROWS), BF16),
            pltpu.VMEM((KEEP, SIDE * ROWS), BF16),
            pltpu.VMEM((GROUPS * COLS, BLOCK), BF16),
            pltpu.VMEM((GROUPS * COLS, BLOCK), BF16),
            pltpu.VMEM((QUARTER, BLOCK), F32),
            dma((T, NX)), dma((T, NX)),
            dma((T, NZ)), dma((T, NZ)),
            dma((T, NZ)), dma((T, NZ)),
            dma((T, NX)), dma((T, NX)),
            dma((SIDE,)), dma((SIDE + 1,)),
            dma((GROUPS,)), dma((GROUPS,)),
            dma((4,)), pltpu.SemaphoreType.REGULAR((4,)),
        ],
        compiler_params=pltpu.CompilerParams(collective_id=0, has_side_effects=True),
    )(prior, analysis, increment, truncation).astype(BF16)


def solution(mesh):
    placed = (
        P("member", None, "band", None),
        P("member", None, "band", None),
        P(None, "band", None),
        P(),
    )
    return jax.shard_map(
        on_device,
        mesh=mesh,
        in_specs=placed,
        out_specs=P("member", None, "band", None),
        check_vma=False,
    )
```

```python
import functools
import math

import jax
import jax.numpy as jnp
from jax import lax
from jax.experimental import pallas as pl
from jax.experimental.pallas import tpu as pltpu
from jax.sharding import PartitionSpec as P

MESH = pl.DeviceIdType.MESH
F32 = jnp.float32
BF16 = jnp.bfloat16

NX, NZ = 4, 4
BANDS, SIDE = 16, 8
LEV, ROWS, NLON = 2, 48, 1536
NLAT = BANDS * ROWS
KEEP = 512
MEMBERS = NX * NZ
QUARTER = LEV * ROWS // NX
R = 8
AT = 6
EARLY = 5
WIDTH = 512
PARTS = NLON // WIDTH
T = QUARTER // R * PARTS
PIECE = WIDTH // NZ
HALF = NLON // 2
GROUPS = 8
WAVES = 64
COLS = 2 * WAVES

RELAX = 0.85
SPREAD_FLOOR = 0.25

COS_TERMS = [(-1.0) ** k / math.factorial(2 * k) for k in range(9)]


def cos_turn(phase, period):
    turns = jnp.floor(phase * (1.0 / period) + 0.5)
    rest = phase - turns * float(period)
    square = rest * rest * ((2.0 * math.pi / period) ** 2)
    total = jnp.full(phase.shape, COS_TERMS[-1], F32)
    for term in COS_TERMS[-2::-1]:
        total = total * square + term
    return total


def halves(values):
    high = values.astype(BF16)
    low = (values - high.astype(F32)).astype(BF16)
    return high, low


def dot(a, b):
    return jnp.dot(a, b, preferred_element_type=F32)


def dot3(a, b):
    return dot(a[0], b[0]) + (dot(a[0], b[1]) + dot(a[1], b[0]))


def iota(shape, dim):
    return lax.broadcasted_iota(jnp.int32, shape, dim)


def inflation(sums):
    count = float(MEMBERS)
    mean_b = sums[0] / count
    mean_a = sums[2] / count
    spread_b = jnp.sqrt(jnp.maximum((sums[1] - count * mean_b * mean_b) / (count - 1), 0.0))
    spread_a = jnp.maximum(
        jnp.sqrt(jnp.maximum((sums[3] - count * mean_a * mean_a) / (count - 1), 0.0)), SPREAD_FLOOR
    )
    factor = 1.0 + RELAX * (spread_b - spread_a) / spread_a
    return factor, mean_b - factor * mean_a


def kernel(
    prior_ref, analysis_ref, inc_ref, trunc_ref, out_ref,
    prior, analysis, inc, trunc, xs, xr, zs, zr, zc, gr, os, cf, ps, pr, kp, kr,
    f_hi, f_lo, c_hi, c_lo, g_hi, g_lo, sm,
    xs_s, xr_s, zs_s, zr_s, gs_s, gr_s, os_s, or_s, cs_s, cr_s, ks_s, kr_s, in_s, reach,
):
    member = lax.axis_index("member")
    band = lax.axis_index("band")
    x, z = member // NZ, lax.rem(member, NZ)
    side, yc = band // SIDE, lax.rem(band, SIDE)
    level = x // 2
    group = lax.rem(x, 2) * NZ + z
    partner = (1 - side) * SIDE + yc
    mate = (level * 2 + 1 - lax.rem(x, 2)) * NZ + z

    def at_x(d):
        return lax.rem(x + d, NX)

    def at_z(d):
        return lax.rem(z + d, NZ)

    def at_band(d):
        return side * SIDE + lax.rem(yc + d, SIDE)

    def group_of(d):
        return lax.rem(group + d, GROUPS)

    def group_dev(g):
        return ((level * 2 + g // NZ) * NZ + lax.rem(g, NZ), band)

    def send(src, dst, send_sem, recv_sem, device):
        copy = pltpu.make_async_remote_copy(
            src_ref=src, dst_ref=dst, send_sem=send_sem, recv_sem=recv_sem,
            device_id=device, device_id_type=MESH,
        )
        copy.start()
        return copy

    def left(src, send_sem):
        pltpu.make_async_remote_copy(
            src_ref=src, dst_ref=src, send_sem=send_sem, recv_sem=send_sem,
            device_id=(member, band), device_id_type=MESH,
        ).wait_send()

    def arrived(dst, recv_sem):
        pltpu.make_async_remote_copy(
            src_ref=dst, dst_ref=dst, send_sem=recv_sem, recv_sem=recv_sem,
            device_id=(member, band), device_id_type=MESH,
        ).wait_recv()

    loads = [
        pltpu.make_async_copy(prior_ref.at[0], prior, in_s.at[0]),
        pltpu.make_async_copy(analysis_ref.at[0], analysis, in_s.at[1]),
        pltpu.make_async_copy(inc_ref.at[level], inc, in_s.at[2]),
        pltpu.make_async_copy(trunc_ref, trunc, in_s.at[3]),
    ]
    for load in loads:
        load.start()

    peers = [(at_x(d) * NZ + z, band) for d in (1, 2, 3)]
    peers += [(member, at_band(d)) for d in range(1, SIDE)]
    barrier = pltpu.get_barrier_semaphore()

    near = ((z > 0, member - 1), (z < NZ - 1, member + 1))
    neighbours = (z > 0).astype(jnp.int32) + (z < NZ - 1).astype(jnp.int32)

    def tell(semaphore):
        for there, device in near:

            @pl.when(there)
            def _():
                pl.semaphore_signal(
                    semaphore, inc=1, device_id=(device, band), device_id_type=MESH
                )

    for peer in peers:
        pl.semaphore_signal(barrier, inc=1, device_id=peer, device_id_type=MESH)
    tell(barrier)

    @pl.when(side == 0)
    def _():
        pl.semaphore_signal(barrier, inc=1, device_id=(member, partner), device_id_type=MESH)

    def wave(g, place):
        return g // 2 * (2 * WAVES) + 2 * place + lax.rem(g, 2)

    def zonal_rows(n, _):
        shape = (64, COLS)
        place = (iota(shape, 0) + n * 64).astype(F32)
        lane = iota(shape, 1)
        number = wave(group, lax.rem(lane, WAVES)).astype(F32)
        shifted = jnp.where(lane >= WAVES, float(NLON // 4), 0.0)
        high, low = halves(cos_turn(place * number - shifted, NLON))
        rows = pl.ds(pl.multiple_of(n * 64, 64), 64)
        f_hi[rows, :] = high
        f_lo[rows, :] = low
        return 0

    def cosine_rows(n, _):
        shape = (16, SIDE * ROWS)
        order = iota(shape, 0) + n * 16
        place = (2 * (iota(shape, 1) + side * SIDE * ROWS) + 1).astype(F32)
        scale = jnp.where(order == 0, math.sqrt(1.0 / NLAT), math.sqrt(2.0 / NLAT))
        high, low = halves(scale * cos_turn(order.astype(F32) * place, 4 * NLAT))
        rows = pl.ds(pl.multiple_of(n * 16, 16), 16)
        c_hi[rows, :] = high
        c_lo[rows, :] = low
        return 0

    def inverse_rows(n, _):
        shape = (16, HALF)
        row = iota(shape, 0) + n * 16
        block = n * 16 // COLS
        g = 2 * lax.rem(block, GROUPS // 2) + block // (GROUPS // 2)
        number = wave(g, lax.rem(row, WAVES))
        shifted = jnp.where(lax.rem(row, COLS) >= WAVES, float(NLON // 4), 0.0)
        weight = jnp.where(number == 0, 1.0 / NLON, 2.0 / NLON)
        place = iota(shape, 1).astype(F32)
        high, low = halves(weight * cos_turn(place * number.astype(F32) - shifted, NLON))
        rows = pl.ds(pl.multiple_of(n * 16, 16), 16)
        g_hi[rows, :] = high
        g_lo[rows, :] = low
        return 0

    cosine_steps = KEEP // 16
    inverse_steps = GROUPS * COLS // 16

    end = (z == 0) | (z == NZ - 1)
    middle = jnp.logical_not(end)
    start = jnp.where(z < 2, 1, 0)
    beyond = jnp.where(z < 2, 1 - z, 5 - z)
    across = 3 - z
    far_end = jnp.where(z == 1, 3, 0)
    other_middle = 3 - z

    def spread_sums(t):
        for d in (1, 3, 2):
            arrived(xr.at[at_x(d), t], xr_s.at[t, at_x(d)])
        b_sum = b_sq = a_sum = a_sq = None
        for d in range(NX):
            b = xs[x, t, 0] if d == 0 else xr[at_x(d), t, 0]
            a = xs[x, t, 1] if d == 0 else xr[at_x(d), t, 1]
            if d == 0:
                b_sum, b_sq, a_sum, a_sq = b, b * b, a, a * a
            else:
                b_sum, b_sq, a_sum, a_sq = b_sum + b, b_sq + b * b, a_sum + a, a_sq + a * a
        for field, total in enumerate((b_sum, b_sq, a_sum, a_sq)):
            for block in range(NZ):
                zs[t, block, field] = total[:, block * PIECE : (block + 1) * PIECE]

        @pl.when(end)
        def _():
            send(
                zs.at[t, pl.ds(start, 3)], zr.at[t, pl.ds(0, 3)], zs_s.at[t, 0], zr_s.at[t, 0],
                (x * NZ + beyond, band),
            )

        @pl.when(middle)
        def _():
            send(
                zs.at[t, beyond], zr.at[t, 0], zs_s.at[t, 0], zr_s.at[t, 0],
                (x * NZ + beyond, band),
            )

    def pass_on(t):
        @pl.when(middle)
        def _():
            arrived(zr.at[t, pl.ds(0, 3)], zr_s.at[t, 0])
            for k, to in enumerate((far_end, other_middle)):
                zc[t, k] = zs[t, to] + zr[t, to - start]
                send(
                    zc.at[t, k], zr.at[t, 3], zs_s.at[t, 1 + k], zr_s.at[t, 1],
                    (x * NZ + to, band),
                )

    def spread_factors(t):
        @pl.when(end)
        def _():
            arrived(zr.at[t, 0], zr_s.at[t, 0])

        arrived(zr.at[t, 3], zr_s.at[t, 1])
        total = zs[t, z] + zr[t, jnp.where(z == 2, 2, 0)] + zr[t, 3]
        factor, shift = inflation([total[field] for field in range(4)])
        gr[t, z, 0] = factor
        gr[t, z, 1] = shift
        for d in (2, 1, 3):
            to = at_z(d)
            send(gr.at[t, z], gr.at[t, z], gs_s.at[t, to], gr_s.at[t, z], (x * NZ + to, band))

    def swap():
        arrived(pr, cr_s.at[SIDE])
        for half in range(2):
            kp[half] = ps[0, half * QUARTER : (half + 1) * QUARTER] + pr[half * QUARTER : (half + 1) * QUARTER]
        kr[group] = kp[group // NZ]
        for d in range(1, GROUPS):
            g = group_of(d)
            send(kp.at[g // NZ], kr.at[group], ks_s.at[d], kr_s.at[group], group_dev(g))

    top = lax.rem(x, 2) * QUARTER

    def update(t):
        for d in (1, 2, 3):
            arrived(gr.at[t, at_z(d)], gr_s.at[t, at_z(d)])
        factor = jnp.concatenate([gr[t, block, 0] for block in range(NZ)], axis=1)
        shift = jnp.concatenate([gr[t, block, 1] for block in range(NZ)], axis=1)
        row, lane = t // PARTS * R, t % PARTS * WIDTH
        shift = shift + sm[row : row + R, lane : lane + WIDTH]
        rows = pl.ds(pl.multiple_of(top + t // PARTS * R, R), R)
        lanes = pl.ds(t % PARTS * WIDTH, WIDTH)
        for d in (2, 1, 3):
            q = at_x(d)
            os[q, t] = shift + factor * xr[q, t, 1]
            send(
                os.at[q, t], out_ref.at[0, level, rows, lanes], os_s.at[t, q], or_s.at[t, x],
                (q * NZ + z, band),
            )
        out_ref[0, level, rows, lanes] = shift + factor * xs[x, t, 1]

    lax.fori_loop(0, NLON // 64, zonal_rows, 0)
    loads[0].wait()
    loads[1].wait()
    for lev in range(LEV):
        for field, ref in enumerate((prior, analysis)):
            values = ref[lev].astype(F32)
            for half in range(2):
                for t in range(T):
                    r = half * QUARTER + t // PARTS * R
                    w = t % PARTS * WIDTH
                    xs[lev * 2 + half, t, field] = values[r : r + R, w : w + WIDTH]

    loads[2].wait()
    loads[3].wait()
    cf[yc] = dot3(halves(inc[...]), (f_hi[...], f_lo[...]))

    pl.semaphore_wait(barrier, len(peers) + neighbours + side)
    for d in (4, 5, 3, 2, 6, 7, 1):
        send(cf.at[yc], cf.at[yc], cs_s.at[d], cr_s.at[yc], (member, at_band(d)))
    for t in range(T):
        for d in (2, 1, 3):
            q = at_x(d)
            send(xs.at[q, t], xr.at[x, t], xs_s.at[t, q], xr_s.at[t, x], (q * NZ + z, band))
    tell(reach.at[0])

    @pl.when(side == 1)
    def _():
        pl.semaphore_signal(reach.at[3], inc=1, device_id=(member, partner), device_id_type=MESH)


    lax.fori_loop(0, cosine_steps, cosine_rows, 0)
    lax.fori_loop(0, 24, inverse_rows, 0)
    pl.semaphore_wait(reach.at[0], neighbours)
    tell(reach.at[1])
    lax.fori_loop(24, 40, inverse_rows, 0)

    for d in range(1, SIDE):
        other = lax.rem(yc + d, SIDE)
        arrived(cf.at[other], cr_s.at[other])
    spec = dot3((c_hi[...], c_lo[...]), halves(cf[...].reshape(SIDE * ROWS, COLS)))
    order = iota((KEEP, COLS), 0)
    number = wave(group, lax.rem(iota((KEEP, COLS), 1), WAVES))
    limit = trunc[level]
    spec = jnp.where(order * order + number * number <= limit * limit, spec, 0.0)
    shape = (2 * ROWS, KEEP)
    row = iota(shape, 0)
    place = row + jnp.where(row < ROWS, band, partner - 1) * ROWS
    order = iota(shape, 1)
    scale = jnp.where(order == 0, math.sqrt(1.0 / NLAT), math.sqrt(2.0 / NLAT))
    back = scale * cos_turn(order.astype(F32) * (2 * place + 1).astype(F32), 4 * NLAT)
    parts = dot3(halves(back), halves(spec))
    ps[0] = parts[:ROWS]
    ps[1] = parts[ROWS:]

    @pl.when(side == 0)
    def _():
        pl.semaphore_wait(reach.at[3], 1)

    send(ps.at[1], pr, cs_s.at[0], cr_s.at[SIDE], (member, partner))
    spread_sums(0)
    pl.semaphore_wait(reach.at[1], neighbours)
    pl.semaphore_signal(reach.at[2], inc=1, device_id=(mate, band), device_id_type=MESH)
    lax.fori_loop(40, 52, inverse_rows, 0)
    spread_sums(1)
    lax.fori_loop(52, inverse_steps, inverse_rows, 0)
    spread_sums(2)
    pass_on(0)
    spread_sums(3)
    pass_on(1)
    pl.semaphore_wait(reach.at[2], 1)
    for t in range(4, T):
        spread_sums(t)
        pass_on(t - 2)
        if t == AT:
            swap()
        if t == T - 1:
            spread_factors(0)
            spread_factors(1)
    pass_on(T - 2)
    spread_factors(2)
    pass_on(T - 1)
    for t in range(3, EARLY):
        spread_factors(t)

    for d in range(1, GROUPS):
        arrived(kr.at[group_of(d)], kr_s.at[group_of(d)])
    even = jnp.concatenate([kr[g] for g in range(0, GROUPS, 2)], axis=1)
    odd = jnp.concatenate([kr[g] for g in range(1, GROUPS, 2)], axis=1)
    depth = GROUPS * COLS // 2
    even = dot3(halves(even), (g_hi[:depth], g_lo[:depth]))
    odd = dot3(halves(odd), (g_hi[depth:], g_lo[depth:]))
    sm[:, :HALF] = even + odd
    sm[:, HALF:] = even - odd

    for t in range(EARLY, T):
        spread_factors(t)
        update(t - EARLY)
    for t in range(T - EARLY, T):
        update(t)

    for t in range(T):
        for d in (1, 2, 3):
            q = at_x(d)
            rows = pl.ds(pl.multiple_of(lax.rem(q, 2) * QUARTER + t // PARTS * R, R), R)
            arrived(
                out_ref.at[0, q // 2, rows, pl.ds(t % PARTS * WIDTH, WIDTH)], or_s.at[t, q]
            )

    for t in range(T):
        for d in (1, 2, 3):
            left(xs.at[at_x(d), t], xs_s.at[t, at_x(d)])
            left(gr.at[t, z], gs_s.at[t, at_z(d)])
            left(os.at[at_x(d), t], os_s.at[t, at_x(d)])
    for d in range(1, SIDE):
        left(cf.at[yc], cs_s.at[d])
        left(kp.at[group_of(d) // NZ], ks_s.at[d])
    left(ps.at[1], cs_s.at[0])

    @pl.when(end)
    def _():
        for t in range(T):
            left(zs.at[t, pl.ds(start, 3)], zs_s.at[t, 0])

    @pl.when(middle)
    def _():
        for t in range(T):
            left(zs.at[t, beyond], zs_s.at[t, 0])
            left(zc.at[t, 0], zs_s.at[t, 1])
            left(zc.at[t, 1], zs_s.at[t, 2])


def on_device(prior, analysis, increment, truncation):
    vmem = pl.BlockSpec(memory_space=pltpu.VMEM)
    hbm = pl.BlockSpec(memory_space=pltpu.HBM)
    dma = pltpu.SemaphoreType.DMA
    return pl.pallas_call(
        kernel,
        out_shape=pltpu.VMEM((1, LEV, ROWS, NLON), F32),
        in_specs=[hbm, hbm, hbm, hbm],
        out_specs=vmem,
        scratch_shapes=[
            pltpu.VMEM((LEV, ROWS, NLON), BF16),
            pltpu.VMEM((LEV, ROWS, NLON), BF16),
            pltpu.VMEM((ROWS, NLON), F32),
            pltpu.SMEM((LEV,), jnp.int32),
            pltpu.VMEM((NX, T, 2, R, WIDTH), F32),
            pltpu.VMEM((NX, T, 2, R, WIDTH), F32),
            pltpu.VMEM((T, NZ, 4, R, PIECE), F32),
            pltpu.VMEM((T, NZ, 4, R, PIECE), F32),
            pltpu.VMEM((T, 2, 4, R, PIECE), F32),
            pltpu.VMEM((T, NZ, 2, R, PIECE), F32),
            pltpu.VMEM((NX, T, R, WIDTH), F32),
            pltpu.VMEM((SIDE, ROWS, COLS), F32),
            pltpu.VMEM((2, ROWS, COLS), F32),
            pltpu.VMEM((ROWS, COLS), F32),
            pltpu.VMEM((2, QUARTER, COLS), F32),
            pltpu.VMEM((GROUPS, QUARTER, COLS), F32),
            pltpu.VMEM((NLON, COLS), BF16),
            pltpu.VMEM((NLON, COLS), BF16),
            pltpu.VMEM((KEEP, SIDE * ROWS), BF16),
            pltpu.VMEM((KEEP, SIDE * ROWS), BF16),
            pltpu.VMEM((GROUPS * COLS, HALF), BF16),
            pltpu.VMEM((GROUPS * COLS, HALF), BF16),
            pltpu.VMEM((QUARTER, NLON), F32),
            dma((T, NX)), dma((T, NX)),
            dma((T, NZ)), dma((T, NZ)),
            dma((T, NZ)), dma((T, NZ)),
            dma((T, NX)), dma((T, NX)),
            dma((SIDE,)), dma((SIDE + 1,)),
            dma((GROUPS,)), dma((GROUPS,)),
            dma((4,)), pltpu.SemaphoreType.REGULAR((4,)),
        ],
        compiler_params=pltpu.CompilerParams(collective_id=0, has_side_effects=True),
    )(prior, analysis, increment, truncation).astype(BF16)


def solution(mesh):
    placed = (
        P("member", None, "band", None),
        P("member", None, "band", None),
        P(None, "band", None),
        P(),
    )
    return jax.shard_map(
        on_device,
        mesh=mesh,
        in_specs=placed,
        out_specs=P("member", None, "band", None),
        check_vma=False,
    )
```

```python
import functools
import math

import jax
import jax.numpy as jnp
from jax import lax
from jax.experimental import pallas as pl
from jax.experimental.pallas import tpu as pltpu
from jax.sharding import PartitionSpec as P

MESH = pl.DeviceIdType.MESH
F32 = jnp.float32
BF16 = jnp.bfloat16

NX, NZ = 4, 4
BANDS, SIDE = 16, 8
LEV, ROWS, NLON = 2, 48, 1536
NLAT = BANDS * ROWS
KEEP = 512
MEMBERS = NX * NZ
QUARTER = LEV * ROWS // NX
R = 8
DIRECT = 6
AT = 6
EARLY = 5
WIDTH = 512
PARTS = NLON // WIDTH
T = QUARTER // R * PARTS
PIECE = WIDTH // NZ
HALF = NLON // 2
GROUPS = 8
WAVES = 64
COLS = 2 * WAVES

RELAX = 0.85
SPREAD_FLOOR = 0.25

COS_TERMS = [(-1.0) ** k / math.factorial(2 * k) for k in range(9)]


def cos_turn(phase, period):
    turns = jnp.floor(phase * (1.0 / period) + 0.5)
    rest = phase - turns * float(period)
    square = rest * rest * ((2.0 * math.pi / period) ** 2)
    total = jnp.full(phase.shape, COS_TERMS[-1], F32)
    for term in COS_TERMS[-2::-1]:
        total = total * square + term
    return total


def halves(values):
    high = values.astype(BF16)
    low = (values - high.astype(F32)).astype(BF16)
    return high, low


def dot(a, b):
    return jnp.dot(a, b, preferred_element_type=F32)


def dot3(a, b):
    return dot(a[0], b[0]) + (dot(a[0], b[1]) + dot(a[1], b[0]))


def iota(shape, dim):
    return lax.broadcasted_iota(jnp.int32, shape, dim)


def inflation(sums):
    count = float(MEMBERS)
    mean_b = sums[0] / count
    mean_a = sums[2] / count
    spread_b = jnp.sqrt(jnp.maximum((sums[1] - count * mean_b * mean_b) / (count - 1), 0.0))
    spread_a = jnp.maximum(
        jnp.sqrt(jnp.maximum((sums[3] - count * mean_a * mean_a) / (count - 1), 0.0)), SPREAD_FLOOR
    )
    factor = 1.0 + RELAX * (spread_b - spread_a) / spread_a
    return factor, mean_b - factor * mean_a


def kernel(
    prior_ref, analysis_ref, inc_ref, trunc_ref, out_ref,
    prior, analysis, inc, trunc, xs, xr, zs, zr, zc, gr, os, cf, ps, pr, kp, kr,
    f_hi, f_lo, c_hi, c_lo, g_hi, g_lo, sm,
    xs_s, xr_s, zs_s, zr_s, gs_s, gr_s, os_s, or_s, cs_s, cr_s, ks_s, kr_s, in_s, reach,
):
    member = lax.axis_index("member")
    band = lax.axis_index("band")
    x, z = member // NZ, lax.rem(member, NZ)
    side, yc = band // SIDE, lax.rem(band, SIDE)
    level = x // 2
    group = lax.rem(x, 2) * NZ + z
    partner = (1 - side) * SIDE + yc
    mate = (level * 2 + 1 - lax.rem(x, 2)) * NZ + z

    def at_x(d):
        return lax.rem(x + d, NX)

    def at_z(d):
        return lax.rem(z + d, NZ)

    def at_band(d):
        return side * SIDE + lax.rem(yc + d, SIDE)

    def group_of(d):
        return lax.rem(group + d, GROUPS)

    def group_dev(g):
        return ((level * 2 + g // NZ) * NZ + lax.rem(g, NZ), band)

    def send(src, dst, send_sem, recv_sem, device):
        copy = pltpu.make_async_remote_copy(
            src_ref=src, dst_ref=dst, send_sem=send_sem, recv_sem=recv_sem,
            device_id=device, device_id_type=MESH,
        )
        copy.start()
        return copy

    def left(src, send_sem):
        pltpu.make_async_remote_copy(
            src_ref=src, dst_ref=src, send_sem=send_sem, recv_sem=send_sem,
            device_id=(member, band), device_id_type=MESH,
        ).wait_send()

    def arrived(dst, recv_sem):
        pltpu.make_async_remote_copy(
            src_ref=dst, dst_ref=dst, send_sem=recv_sem, recv_sem=recv_sem,
            device_id=(member, band), device_id_type=MESH,
        ).wait_recv()

    loads = [
        pltpu.make_async_copy(prior_ref.at[0], prior, in_s.at[0]),
        pltpu.make_async_copy(analysis_ref.at[0], analysis, in_s.at[1]),
        pltpu.make_async_copy(inc_ref.at[level], inc, in_s.at[2]),
        pltpu.make_async_copy(trunc_ref, trunc, in_s.at[3]),
    ]
    for load in loads:
        load.start()

    peers = [(at_x(d) * NZ + z, band) for d in (1, 2, 3)]
    peers += [(member, at_band(d)) for d in range(1, SIDE)]
    barrier = pltpu.get_barrier_semaphore()

    near = ((z > 0, member - 1), (z < NZ - 1, member + 1))
    neighbours = (z > 0).astype(jnp.int32) + (z < NZ - 1).astype(jnp.int32)

    def tell(semaphore):
        for there, device in near:

            @pl.when(there)
            def _():
                pl.semaphore_signal(
                    semaphore, inc=1, device_id=(device, band), device_id_type=MESH
                )

    for peer in peers:
        pl.semaphore_signal(barrier, inc=1, device_id=peer, device_id_type=MESH)
    tell(barrier)

    @pl.when(side == 0)
    def _():
        pl.semaphore_signal(barrier, inc=1, device_id=(member, partner), device_id_type=MESH)

    def wave(g, place):
        return g // 2 * (2 * WAVES) + 2 * place + lax.rem(g, 2)

    def zonal_rows(n, _):
        shape = (64, COLS)
        place = (iota(shape, 0) + n * 64).astype(F32)
        lane = iota(shape, 1)
        number = wave(group, lax.rem(lane, WAVES)).astype(F32)
        shifted = jnp.where(lane >= WAVES, float(NLON // 4), 0.0)
        high, low = halves(cos_turn(place * number - shifted, NLON))
        rows = pl.ds(pl.multiple_of(n * 64, 64), 64)
        f_hi[rows, :] = high
        f_lo[rows, :] = low
        return 0

    def cosine_rows(n, _):
        shape = (16, SIDE * ROWS)
        order = iota(shape, 0) + n * 16
        place = (2 * (iota(shape, 1) + side * SIDE * ROWS) + 1).astype(F32)
        scale = jnp.where(order == 0, math.sqrt(1.0 / NLAT), math.sqrt(2.0 / NLAT))
        high, low = halves(scale * cos_turn(order.astype(F32) * place, 4 * NLAT))
        rows = pl.ds(pl.multiple_of(n * 16, 16), 16)
        c_hi[rows, :] = high
        c_lo[rows, :] = low
        return 0

    def inverse_rows(n, _):
        shape = (16, HALF)
        row = iota(shape, 0) + n * 16
        block = n * 16 // COLS
        g = 2 * lax.rem(block, GROUPS // 2) + block // (GROUPS // 2)
        number = wave(g, lax.rem(row, WAVES))
        shifted = jnp.where(lax.rem(row, COLS) >= WAVES, float(NLON // 4), 0.0)
        weight = jnp.where(number == 0, 1.0 / NLON, 2.0 / NLON)
        place = iota(shape, 1).astype(F32)
        high, low = halves(weight * cos_turn(place * number.astype(F32) - shifted, NLON))
        rows = pl.ds(pl.multiple_of(n * 16, 16), 16)
        g_hi[rows, :] = high
        g_lo[rows, :] = low
        return 0

    cosine_steps = KEEP // 16
    inverse_steps = GROUPS * COLS // 16

    end = (z == 0) | (z == NZ - 1)
    middle = jnp.logical_not(end)
    start = jnp.where(z < 2, 1, 0)
    beyond = jnp.where(z < 2, 1 - z, 5 - z)
    across = 3 - z
    far_end = jnp.where(z == 1, 3, 0)
    other_middle = 3 - z

    def spread_sums(t):
        for d in (1, 3, 2):
            arrived(xr.at[at_x(d), t], xr_s.at[t, at_x(d)])
        b_sum = b_sq = a_sum = a_sq = None
        for d in range(NX):
            b = xs[x, t, 0] if d == 0 else xr[at_x(d), t, 0]
            a = xs[x, t, 1] if d == 0 else xr[at_x(d), t, 1]
            if d == 0:
                b_sum, b_sq, a_sum, a_sq = b, b * b, a, a * a
            else:
                b_sum, b_sq, a_sum, a_sq = b_sum + b, b_sq + b * b, a_sum + a, a_sq + a * a
        for field, total in enumerate((b_sum, b_sq, a_sum, a_sq)):
            for block in range(NZ):
                zs[t, block, field] = total[:, block * PIECE : (block + 1) * PIECE]

        if t < DIRECT:
            for d in (2, 1, 3):
                to = at_z(d)
                send(zs.at[t, to], zr.at[t, z], zs_s.at[t, d], zr_s.at[t, z], (x * NZ + to, band))
            return

        @pl.when(end)
        def _():
            far = jnp.where(z == 0, 2, 0)
            send(
                zs.at[t, pl.ds(far, 2)], zr.at[t, pl.ds(far - start, 2)], zs_s.at[t, 0],
                zr_s.at[t, 0], (x * NZ + beyond, band),
            )
            send(
                zs.at[t, beyond], zr.at[t, beyond - start], zs_s.at[t, 1], zr_s.at[t, 2],
                (x * NZ + beyond, band),
            )

        @pl.when(middle)
        def _():
            send(
                zs.at[t, beyond], zr.at[t, 0], zs_s.at[t, 0], zr_s.at[t, 0],
                (x * NZ + beyond, band),
            )

    def pass_on(t):
        if t < DIRECT:
            return

        @pl.when(middle)
        def _():
            arrived(zr.at[t, pl.ds(jnp.where(z == 1, 1, 0), 2)], zr_s.at[t, 0])
            for k, to in enumerate((far_end, other_middle)):
                zc[t, k] = zs[t, to] + zr[t, to - start]
                send(
                    zc.at[t, k], zr.at[t, 3], zs_s.at[t, 1 + k], zr_s.at[t, 1],
                    (x * NZ + to, band),
                )

    def spread_factors(t):
        if t < DIRECT:
            total = zs[t, z]
            for d in (1, 3, 2):
                arrived(zr.at[t, at_z(d)], zr_s.at[t, at_z(d)])
                total = total + zr[t, at_z(d)]
        else:
            @pl.when(end)
            def _():
                arrived(zr.at[t, 0], zr_s.at[t, 0])

            @pl.when(middle)
            def _():
                arrived(zr.at[t, jnp.where(z == 2, 2, 0)], zr_s.at[t, 2])

            arrived(zr.at[t, 3], zr_s.at[t, 1])
            total = zs[t, z] + zr[t, jnp.where(z == 2, 2, 0)] + zr[t, 3]
        factor, shift = inflation([total[field] for field in range(4)])
        gr[t, z, 0] = factor
        gr[t, z, 1] = shift
        for d in (2, 1, 3):
            to = at_z(d)
            send(gr.at[t, z], gr.at[t, z], gs_s.at[t, to], gr_s.at[t, z], (x * NZ + to, band))

    def swap():
        arrived(pr, cr_s.at[SIDE])
        for half in range(2):
            kp[half] = ps[0, half * QUARTER : (half + 1) * QUARTER] + pr[half * QUARTER : (half + 1) * QUARTER]
        kr[group] = kp[group // NZ]
        for d in range(1, GROUPS):
            g = group_of(d)
            send(kp.at[g // NZ], kr.at[group], ks_s.at[d], kr_s.at[group], group_dev(g))

    top = lax.rem(x, 2) * QUARTER

    def update(t):
        for d in (1, 2, 3):
            arrived(gr.at[t, at_z(d)], gr_s.at[t, at_z(d)])
        factor = jnp.concatenate([gr[t, block, 0] for block in range(NZ)], axis=1)
        shift = jnp.concatenate([gr[t, block, 1] for block in range(NZ)], axis=1)
        row, lane = t // PARTS * R, t % PARTS * WIDTH
        shift = shift + sm[row : row + R, lane : lane + WIDTH]
        rows = pl.ds(pl.multiple_of(top + t // PARTS * R, R), R)
        lanes = pl.ds(t % PARTS * WIDTH, WIDTH)
        for d in (2, 1, 3):
            q = at_x(d)
            os[q, t] = shift + factor * xr[q, t, 1]
            send(
                os.at[q, t], out_ref.at[0, level, rows, lanes], os_s.at[t, q], or_s.at[t, x],
                (q * NZ + z, band),
            )
        out_ref[0, level, rows, lanes] = shift + factor * xs[x, t, 1]

    lax.fori_loop(0, NLON // 64, zonal_rows, 0)
    loads[0].wait()
    loads[1].wait()
    for lev in range(LEV):
        for field, ref in enumerate((prior, analysis)):
            values = ref[lev].astype(F32)
            for half in range(2):
                for t in range(T):
                    r = half * QUARTER + t // PARTS * R
                    w = t % PARTS * WIDTH
                    xs[lev * 2 + half, t, field] = values[r : r + R, w : w + WIDTH]

    loads[2].wait()
    loads[3].wait()
    cf[yc] = dot3(halves(inc[...]), (f_hi[...], f_lo[...]))

    pl.semaphore_wait(barrier, len(peers) + neighbours + side)
    for d in (4, 5, 3, 2, 6, 7, 1):
        send(cf.at[yc], cf.at[yc], cs_s.at[d], cr_s.at[yc], (member, at_band(d)))
    for t in range(T):
        for d in (2, 1, 3):
            q = at_x(d)
            send(xs.at[q, t], xr.at[x, t], xs_s.at[t, q], xr_s.at[t, x], (q * NZ + z, band))
    tell(reach.at[0])

    @pl.when(side == 1)
    def _():
        pl.semaphore_signal(reach.at[3], inc=1, device_id=(member, partner), device_id_type=MESH)


    lax.fori_loop(0, cosine_steps, cosine_rows, 0)
    lax.fori_loop(0, 24, inverse_rows, 0)
    pl.semaphore_wait(reach.at[0], neighbours)
    tell(reach.at[1])
    lax.fori_loop(24, 40, inverse_rows, 0)

    for d in range(1, SIDE):
        other = lax.rem(yc + d, SIDE)
        arrived(cf.at[other], cr_s.at[other])
    spec = dot3((c_hi[...], c_lo[...]), halves(cf[...].reshape(SIDE * ROWS, COLS)))
    pl.semaphore_wait(reach.at[1], neighbours)
    spread_sums(0)
    order = iota((KEEP, COLS), 0)
    number = wave(group, lax.rem(iota((KEEP, COLS), 1), WAVES))
    limit = trunc[level]
    spec = jnp.where(order * order + number * number <= limit * limit, spec, 0.0)
    shape = (2 * ROWS, KEEP)
    row = iota(shape, 0)
    place = row + jnp.where(row < ROWS, band, partner - 1) * ROWS
    order = iota(shape, 1)
    scale = jnp.where(order == 0, math.sqrt(1.0 / NLAT), math.sqrt(2.0 / NLAT))
    back = scale * cos_turn(order.astype(F32) * (2 * place + 1).astype(F32), 4 * NLAT)
    parts = dot3(halves(back), halves(spec))
    ps[0] = parts[:ROWS]
    ps[1] = parts[ROWS:]

    @pl.when(side == 0)
    def _():
        pl.semaphore_wait(reach.at[3], 1)

    send(ps.at[1], pr, cs_s.at[0], cr_s.at[SIDE], (member, partner))
    pl.semaphore_signal(reach.at[2], inc=1, device_id=(mate, band), device_id_type=MESH)
    spread_sums(1)
    lax.fori_loop(40, 48, inverse_rows, 0)
    spread_sums(2)
    pass_on(0)
    lax.fori_loop(48, 56, inverse_rows, 0)
    spread_sums(3)
    pass_on(1)
    lax.fori_loop(56, inverse_steps, inverse_rows, 0)
    pl.semaphore_wait(reach.at[2], 1)
    for t in range(4, T):
        spread_sums(t)
        pass_on(t - 2)
        if t == AT:
            swap()
        if t == T - 1:
            spread_factors(0)
            spread_factors(1)
    pass_on(T - 2)
    spread_factors(2)
    pass_on(T - 1)
    for t in range(3, EARLY):
        spread_factors(t)

    for d in range(1, GROUPS):
        arrived(kr.at[group_of(d)], kr_s.at[group_of(d)])
    even = jnp.concatenate([kr[g] for g in range(0, GROUPS, 2)], axis=1)
    odd = jnp.concatenate([kr[g] for g in range(1, GROUPS, 2)], axis=1)
    depth = GROUPS * COLS // 2
    even = dot3(halves(even), (g_hi[:depth], g_lo[:depth]))
    odd = dot3(halves(odd), (g_hi[depth:], g_lo[depth:]))
    sm[:, :HALF] = even + odd
    sm[:, HALF:] = even - odd

    for t in range(EARLY, T):
        spread_factors(t)
        update(t - EARLY)
    for t in range(T - EARLY, T):
        update(t)

    for t in range(T):
        for d in (1, 2, 3):
            q = at_x(d)
            rows = pl.ds(pl.multiple_of(lax.rem(q, 2) * QUARTER + t // PARTS * R, R), R)
            arrived(
                out_ref.at[0, q // 2, rows, pl.ds(t % PARTS * WIDTH, WIDTH)], or_s.at[t, q]
            )

    for t in range(T):
        for d in (1, 2, 3):
            left(xs.at[at_x(d), t], xs_s.at[t, at_x(d)])
            left(gr.at[t, z], gs_s.at[t, at_z(d)])
            left(os.at[at_x(d), t], os_s.at[t, at_x(d)])
    for d in range(1, SIDE):
        left(cf.at[yc], cs_s.at[d])
        left(kp.at[group_of(d) // NZ], ks_s.at[d])
    left(ps.at[1], cs_s.at[0])

    for t in range(DIRECT):
        for d in (1, 2, 3):
            left(zs.at[t, at_z(d)], zs_s.at[t, d])

    @pl.when(end)
    def _():
        for t in range(DIRECT, T):
            left(zs.at[t, pl.ds(jnp.where(z == 0, 2, 0), 2)], zs_s.at[t, 0])
            left(zs.at[t, beyond], zs_s.at[t, 1])

    @pl.when(middle)
    def _():
        for t in range(DIRECT, T):
            left(zs.at[t, beyond], zs_s.at[t, 0])
            left(zc.at[t, 0], zs_s.at[t, 1])
            left(zc.at[t, 1], zs_s.at[t, 2])


def on_device(prior, analysis, increment, truncation):
    vmem = pl.BlockSpec(memory_space=pltpu.VMEM)
    hbm = pl.BlockSpec(memory_space=pltpu.HBM)
    dma = pltpu.SemaphoreType.DMA
    return pl.pallas_call(
        kernel,
        out_shape=pltpu.VMEM((1, LEV, ROWS, NLON), F32),
        in_specs=[hbm, hbm, hbm, hbm],
        out_specs=vmem,
        scratch_shapes=[
            pltpu.VMEM((LEV, ROWS, NLON), BF16),
            pltpu.VMEM((LEV, ROWS, NLON), BF16),
            pltpu.VMEM((ROWS, NLON), F32),
            pltpu.SMEM((LEV,), jnp.int32),
            pltpu.VMEM((NX, T, 2, R, WIDTH), F32),
            pltpu.VMEM((NX, T, 2, R, WIDTH), F32),
            pltpu.VMEM((T, NZ, 4, R, PIECE), F32),
            pltpu.VMEM((T, NZ, 4, R, PIECE), F32),
            pltpu.VMEM((T, 2, 4, R, PIECE), F32),
            pltpu.VMEM((T, NZ, 2, R, PIECE), F32),
            pltpu.VMEM((NX, T, R, WIDTH), F32),
            pltpu.VMEM((SIDE, ROWS, COLS), F32),
            pltpu.VMEM((2, ROWS, COLS), F32),
            pltpu.VMEM((ROWS, COLS), F32),
            pltpu.VMEM((2, QUARTER, COLS), F32),
            pltpu.VMEM((GROUPS, QUARTER, COLS), F32),
            pltpu.VMEM((NLON, COLS), BF16),
            pltpu.VMEM((NLON, COLS), BF16),
            pltpu.VMEM((KEEP, SIDE * ROWS), BF16),
            pltpu.VMEM((KEEP, SIDE * ROWS), BF16),
            pltpu.VMEM((GROUPS * COLS, HALF), BF16),
            pltpu.VMEM((GROUPS * COLS, HALF), BF16),
            pltpu.VMEM((QUARTER, NLON), F32),
            dma((T, NX)), dma((T, NX)),
            dma((T, NZ)), dma((T, NZ)),
            dma((T, NZ)), dma((T, NZ)),
            dma((T, NX)), dma((T, NX)),
            dma((SIDE,)), dma((SIDE + 1,)),
            dma((GROUPS,)), dma((GROUPS,)),
            dma((4,)), pltpu.SemaphoreType.REGULAR((4,)),
        ],
        compiler_params=pltpu.CompilerParams(collective_id=0, has_side_effects=True),
    )(prior, analysis, increment, truncation).astype(BF16)


def solution(mesh):
    placed = (
        P("member", None, "band", None),
        P("member", None, "band", None),
        P(None, "band", None),
        P(),
    )
    return jax.shard_map(
        on_device,
        mesh=mesh,
        in_specs=placed,
        out_specs=P("member", None, "band", None),
        check_vma=False,
    )
```

```python
import functools
import math

import jax
import jax.numpy as jnp
from jax import lax
from jax.experimental import pallas as pl
from jax.experimental.pallas import tpu as pltpu
from jax.sharding import PartitionSpec as P

MESH = pl.DeviceIdType.MESH
F32 = jnp.float32
BF16 = jnp.bfloat16

NX, NZ = 4, 4
BANDS, SIDE = 16, 8
LEV, ROWS, NLON = 2, 48, 1536
NLAT = BANDS * ROWS
KEEP = 512
MEMBERS = NX * NZ
QUARTER = LEV * ROWS // NX
R = 8
COMBINED = (5, 6, 7, 8)
LAGP = 3
AT = 6
EARLY = 5
WIDTH = 512
PARTS = NLON // WIDTH
T = QUARTER // R * PARTS
PIECE = WIDTH // NZ
HALF = NLON // 2
GROUPS = 8
WAVES = 64
COLS = 2 * WAVES

RELAX = 0.85
SPREAD_FLOOR = 0.25

COS_TERMS = [(-1.0) ** k / math.factorial(2 * k) for k in range(9)]


def cos_turn(phase, period):
    turns = jnp.floor(phase * (1.0 / period) + 0.5)
    rest = phase - turns * float(period)
    square = rest * rest * ((2.0 * math.pi / period) ** 2)
    total = jnp.full(phase.shape, COS_TERMS[-1], F32)
    for term in COS_TERMS[-2::-1]:
        total = total * square + term
    return total


def halves(values):
    high = values.astype(BF16)
    low = (values - high.astype(F32)).astype(BF16)
    return high, low


def dot(a, b):
    return jnp.dot(a, b, preferred_element_type=F32)


def dot3(a, b):
    return dot(a[0], b[0]) + (dot(a[0], b[1]) + dot(a[1], b[0]))


def iota(shape, dim):
    return lax.broadcasted_iota(jnp.int32, shape, dim)


def inflation(sums):
    count = float(MEMBERS)
    mean_b = sums[0] / count
    mean_a = sums[2] / count
    spread_b = jnp.sqrt(jnp.maximum((sums[1] - count * mean_b * mean_b) / (count - 1), 0.0))
    spread_a = jnp.maximum(
        jnp.sqrt(jnp.maximum((sums[3] - count * mean_a * mean_a) / (count - 1), 0.0)), SPREAD_FLOOR
    )
    factor = 1.0 + RELAX * (spread_b - spread_a) / spread_a
    return factor, mean_b - factor * mean_a


def kernel(
    prior_ref, analysis_ref, inc_ref, trunc_ref, out_ref,
    prior, analysis, inc, trunc, xs, xr, zs, zr, zc, gr, os, cf, ps, pr, kp, kr,
    f_hi, f_lo, c_hi, c_lo, g_hi, g_lo, sm,
    xs_s, xr_s, zs_s, zr_s, gs_s, gr_s, os_s, or_s, cs_s, cr_s, ks_s, kr_s, in_s, reach,
):
    member = lax.axis_index("member")
    band = lax.axis_index("band")
    x, z = member // NZ, lax.rem(member, NZ)
    side, yc = band // SIDE, lax.rem(band, SIDE)
    level = x // 2
    group = lax.rem(x, 2) * NZ + z
    partner = (1 - side) * SIDE + yc
    mate = (level * 2 + 1 - lax.rem(x, 2)) * NZ + z

    def at_x(d):
        return lax.rem(x + d, NX)

    def at_z(d):
        return lax.rem(z + d, NZ)

    def at_band(d):
        return side * SIDE + lax.rem(yc + d, SIDE)

    def group_of(d):
        return lax.rem(group + d, GROUPS)

    def group_dev(g):
        return ((level * 2 + g // NZ) * NZ + lax.rem(g, NZ), band)

    def send(src, dst, send_sem, recv_sem, device):
        copy = pltpu.make_async_remote_copy(
            src_ref=src, dst_ref=dst, send_sem=send_sem, recv_sem=recv_sem,
            device_id=device, device_id_type=MESH,
        )
        copy.start()
        return copy

    def left(src, send_sem):
        pltpu.make_async_remote_copy(
            src_ref=src, dst_ref=src, send_sem=send_sem, recv_sem=send_sem,
            device_id=(member, band), device_id_type=MESH,
        ).wait_send()

    def arrived(dst, recv_sem):
        pltpu.make_async_remote_copy(
            src_ref=dst, dst_ref=dst, send_sem=recv_sem, recv_sem=recv_sem,
            device_id=(member, band), device_id_type=MESH,
        ).wait_recv()

    loads = [
        pltpu.make_async_copy(prior_ref.at[0], prior, in_s.at[0]),
        pltpu.make_async_copy(analysis_ref.at[0], analysis, in_s.at[1]),
        pltpu.make_async_copy(inc_ref.at[level], inc, in_s.at[2]),
        pltpu.make_async_copy(trunc_ref, trunc, in_s.at[3]),
    ]
    for load in loads:
        load.start()

    peers = [(at_x(d) * NZ + z, band) for d in (1, 2, 3)]
    peers += [(member, at_band(d)) for d in range(1, SIDE)]
    barrier = pltpu.get_barrier_semaphore()

    near = ((z > 0, member - 1), (z < NZ - 1, member + 1))
    neighbours = (z > 0).astype(jnp.int32) + (z < NZ - 1).astype(jnp.int32)

    def tell(semaphore):
        for there, device in near:

            @pl.when(there)
            def _():
                pl.semaphore_signal(
                    semaphore, inc=1, device_id=(device, band), device_id_type=MESH
                )

    for peer in peers:
        pl.semaphore_signal(barrier, inc=1, device_id=peer, device_id_type=MESH)
    tell(barrier)

    @pl.when(side == 0)
    def _():
        pl.semaphore_signal(barrier, inc=1, device_id=(member, partner), device_id_type=MESH)

    def wave(g, place):
        return g // 2 * (2 * WAVES) + 2 * place + lax.rem(g, 2)

    def zonal_rows(n, _):
        shape = (64, COLS)
        place = (iota(shape, 0) + n * 64).astype(F32)
        lane = iota(shape, 1)
        number = wave(group, lax.rem(lane, WAVES)).astype(F32)
        shifted = jnp.where(lane >= WAVES, float(NLON // 4), 0.0)
        high, low = halves(cos_turn(place * number - shifted, NLON))
        rows = pl.ds(pl.multiple_of(n * 64, 64), 64)
        f_hi[rows, :] = high
        f_lo[rows, :] = low
        return 0

    def cosine_rows(n, _):
        shape = (16, SIDE * ROWS)
        order = iota(shape, 0) + n * 16
        place = (2 * (iota(shape, 1) + side * SIDE * ROWS) + 1).astype(F32)
        scale = jnp.where(order == 0, math.sqrt(1.0 / NLAT), math.sqrt(2.0 / NLAT))
        high, low = halves(scale * cos_turn(order.astype(F32) * place, 4 * NLAT))
        rows = pl.ds(pl.multiple_of(n * 16, 16), 16)
        c_hi[rows, :] = high
        c_lo[rows, :] = low
        return 0

    def inverse_rows(n, _):
        shape = (16, HALF)
        row = iota(shape, 0) + n * 16
        block = n * 16 // COLS
        g = 2 * lax.rem(block, GROUPS // 2) + block // (GROUPS // 2)
        number = wave(g, lax.rem(row, WAVES))
        shifted = jnp.where(lax.rem(row, COLS) >= WAVES, float(NLON // 4), 0.0)
        weight = jnp.where(number == 0, 1.0 / NLON, 2.0 / NLON)
        place = iota(shape, 1).astype(F32)
        high, low = halves(weight * cos_turn(place * number.astype(F32) - shifted, NLON))
        rows = pl.ds(pl.multiple_of(n * 16, 16), 16)
        g_hi[rows, :] = high
        g_lo[rows, :] = low
        return 0

    cosine_steps = KEEP // 16
    inverse_steps = GROUPS * COLS // 16

    end = (z == 0) | (z == NZ - 1)
    middle = jnp.logical_not(end)
    start = jnp.where(z < 2, 1, 0)
    beyond = jnp.where(z < 2, 1 - z, 5 - z)
    across = 3 - z
    far_end = jnp.where(z == 1, 3, 0)
    other_middle = 3 - z

    def spread_sums(t):
        for d in (1, 3, 2):
            arrived(xr.at[at_x(d), t], xr_s.at[t, at_x(d)])
        b_sum = b_sq = a_sum = a_sq = None
        for d in range(NX):
            b = xs[x, t, 0] if d == 0 else xr[at_x(d), t, 0]
            a = xs[x, t, 1] if d == 0 else xr[at_x(d), t, 1]
            if d == 0:
                b_sum, b_sq, a_sum, a_sq = b, b * b, a, a * a
            else:
                b_sum, b_sq, a_sum, a_sq = b_sum + b, b_sq + b * b, a_sum + a, a_sq + a * a
        for field, total in enumerate((b_sum, b_sq, a_sum, a_sq)):
            for block in range(NZ):
                zs[t, block, field] = total[:, block * PIECE : (block + 1) * PIECE]

        if t not in COMBINED:
            for d in (2, 1, 3):
                to = at_z(d)
                send(zs.at[t, to], zr.at[t, z], zs_s.at[t, d], zr_s.at[t, z], (x * NZ + to, band))
            return

        @pl.when(end)
        def _():
            far = jnp.where(z == 0, 2, 0)
            send(
                zs.at[t, pl.ds(far, 2)], zr.at[t, pl.ds(far - start, 2)], zs_s.at[t, 0],
                zr_s.at[t, 0], (x * NZ + beyond, band),
            )
            send(
                zs.at[t, beyond], zr.at[t, beyond - start], zs_s.at[t, 1], zr_s.at[t, 2],
                (x * NZ + beyond, band),
            )

        @pl.when(middle)
        def _():
            send(
                zs.at[t, beyond], zr.at[t, 0], zs_s.at[t, 0], zr_s.at[t, 0],
                (x * NZ + beyond, band),
            )

    def pass_on(t):
        if t not in COMBINED:
            return

        @pl.when(middle)
        def _():
            arrived(zr.at[t, pl.ds(jnp.where(z == 1, 1, 0), 2)], zr_s.at[t, 0])
            for k, to in enumerate((far_end, other_middle)):
                zc[t, k] = zs[t, to] + zr[t, to - start]
                send(
                    zc.at[t, k], zr.at[t, 3], zs_s.at[t, 1 + k], zr_s.at[t, 1],
                    (x * NZ + to, band),
                )

    def spread_factors(t):
        if t not in COMBINED:
            total = zs[t, z]
            for d in (1, 3, 2):
                arrived(zr.at[t, at_z(d)], zr_s.at[t, at_z(d)])
                total = total + zr[t, at_z(d)]
        else:
            @pl.when(end)
            def _():
                arrived(zr.at[t, 0], zr_s.at[t, 0])

            @pl.when(middle)
            def _():
                arrived(zr.at[t, jnp.where(z == 2, 2, 0)], zr_s.at[t, 2])

            arrived(zr.at[t, 3], zr_s.at[t, 1])
            total = zs[t, z] + zr[t, jnp.where(z == 2, 2, 0)] + zr[t, 3]
        factor, shift = inflation([total[field] for field in range(4)])
        gr[t, z, 0] = factor
        gr[t, z, 1] = shift
        for d in (2, 1, 3):
            to = at_z(d)
            send(gr.at[t, z], gr.at[t, z], gs_s.at[t, to], gr_s.at[t, z], (x * NZ + to, band))

    def swap():
        arrived(pr, cr_s.at[SIDE])
        for half in range(2):
            kp[half] = ps[0, half * QUARTER : (half + 1) * QUARTER] + pr[half * QUARTER : (half + 1) * QUARTER]
        kr[group] = kp[group // NZ]
        for d in range(1, GROUPS):
            g = group_of(d)
            send(kp.at[g // NZ], kr.at[group], ks_s.at[d], kr_s.at[group], group_dev(g))

    top = lax.rem(x, 2) * QUARTER

    def update(t):
        for d in (1, 2, 3):
            arrived(gr.at[t, at_z(d)], gr_s.at[t, at_z(d)])
        factor = jnp.concatenate([gr[t, block, 0] for block in range(NZ)], axis=1)
        shift = jnp.concatenate([gr[t, block, 1] for block in range(NZ)], axis=1)
        row, lane = t // PARTS * R, t % PARTS * WIDTH
        shift = shift + sm[row : row + R, lane : lane + WIDTH]
        rows = pl.ds(pl.multiple_of(top + t // PARTS * R, R), R)
        lanes = pl.ds(t % PARTS * WIDTH, WIDTH)
        for d in (2, 1, 3):
            q = at_x(d)
            os[q, t] = shift + factor * xr[q, t, 1]
            send(
                os.at[q, t], out_ref.at[0, level, rows, lanes], os_s.at[t, q], or_s.at[t, x],
                (q * NZ + z, band),
            )
        out_ref[0, level, rows, lanes] = shift + factor * xs[x, t, 1]

    lax.fori_loop(0, NLON // 64, zonal_rows, 0)
    loads[0].wait()
    loads[1].wait()
    for lev in range(LEV):
        for field, ref in enumerate((prior, analysis)):
            values = ref[lev].astype(F32)
            for half in range(2):
                for t in range(T):
                    r = half * QUARTER + t // PARTS * R
                    w = t % PARTS * WIDTH
                    xs[lev * 2 + half, t, field] = values[r : r + R, w : w + WIDTH]

    loads[2].wait()
    loads[3].wait()
    cf[yc] = dot3(halves(inc[...]), (f_hi[...], f_lo[...]))

    pl.semaphore_wait(barrier, len(peers) + neighbours + side)
    for d in (4, 5, 3, 2, 6, 7, 1):
        send(cf.at[yc], cf.at[yc], cs_s.at[d], cr_s.at[yc], (member, at_band(d)))
    for t in range(T):
        for d in (2, 1, 3):
            q = at_x(d)
            send(xs.at[q, t], xr.at[x, t], xs_s.at[t, q], xr_s.at[t, x], (q * NZ + z, band))
    tell(reach.at[0])

    @pl.when(side == 1)
    def _():
        pl.semaphore_signal(reach.at[3], inc=1, device_id=(member, partner), device_id_type=MESH)


    lax.fori_loop(0, cosine_steps, cosine_rows, 0)
    lax.fori_loop(0, 24, inverse_rows, 0)
    pl.semaphore_wait(reach.at[0], neighbours)
    tell(reach.at[1])
    lax.fori_loop(24, 40, inverse_rows, 0)

    for d in range(1, SIDE):
        other = lax.rem(yc + d, SIDE)
        arrived(cf.at[other], cr_s.at[other])
    spec = dot3((c_hi[...], c_lo[...]), halves(cf[...].reshape(SIDE * ROWS, COLS)))
    pl.semaphore_wait(reach.at[1], neighbours)
    spread_sums(0)
    order = iota((KEEP, COLS), 0)
    number = wave(group, lax.rem(iota((KEEP, COLS), 1), WAVES))
    limit = trunc[level]
    spec = jnp.where(order * order + number * number <= limit * limit, spec, 0.0)
    shape = (2 * ROWS, KEEP)
    row = iota(shape, 0)
    place = row + jnp.where(row < ROWS, band, partner - 1) * ROWS
    order = iota(shape, 1)
    scale = jnp.where(order == 0, math.sqrt(1.0 / NLAT), math.sqrt(2.0 / NLAT))
    back = scale * cos_turn(order.astype(F32) * (2 * place + 1).astype(F32), 4 * NLAT)
    parts = dot3(halves(back), halves(spec))
    ps[0] = parts[:ROWS]
    ps[1] = parts[ROWS:]

    @pl.when(side == 0)
    def _():
        pl.semaphore_wait(reach.at[3], 1)

    send(ps.at[1], pr, cs_s.at[0], cr_s.at[SIDE], (member, partner))
    pl.semaphore_signal(reach.at[2], inc=1, device_id=(mate, band), device_id_type=MESH)
    spread_sums(1)
    lax.fori_loop(40, 48, inverse_rows, 0)
    spread_sums(2)
    lax.fori_loop(48, 56, inverse_rows, 0)
    spread_sums(3)
    for t in range(4 - LAGP):
        pass_on(t)
    lax.fori_loop(56, inverse_steps, inverse_rows, 0)
    pl.semaphore_wait(reach.at[2], 1)
    for t in range(4, T):
        spread_sums(t)
        pass_on(t - LAGP)
        if t == AT:
            swap()
        if t == T - 1:
            spread_factors(0)
            spread_factors(1)
    for t in range(T - LAGP, T - 1):
        pass_on(t)
    spread_factors(2)
    pass_on(T - 1)
    for t in range(3, EARLY):
        spread_factors(t)

    for d in range(1, GROUPS):
        arrived(kr.at[group_of(d)], kr_s.at[group_of(d)])
    even = jnp.concatenate([kr[g] for g in range(0, GROUPS, 2)], axis=1)
    odd = jnp.concatenate([kr[g] for g in range(1, GROUPS, 2)], axis=1)
    depth = GROUPS * COLS // 2
    even = dot3(halves(even), (g_hi[:depth], g_lo[:depth]))
    odd = dot3(halves(odd), (g_hi[depth:], g_lo[depth:]))
    sm[:, :HALF] = even + odd
    sm[:, HALF:] = even - odd

    for t in range(EARLY, T):
        spread_factors(t)
        update(t - EARLY)
    for t in range(T - EARLY, T):
        update(t)

    for t in range(T):
        for d in (1, 2, 3):
            q = at_x(d)
            rows = pl.ds(pl.multiple_of(lax.rem(q, 2) * QUARTER + t // PARTS * R, R), R)
            arrived(
                out_ref.at[0, q // 2, rows, pl.ds(t % PARTS * WIDTH, WIDTH)], or_s.at[t, q]
            )

    for t in range(T):
        for d in (1, 2, 3):
            left(xs.at[at_x(d), t], xs_s.at[t, at_x(d)])
            left(gr.at[t, z], gs_s.at[t, at_z(d)])
            left(os.at[at_x(d), t], os_s.at[t, at_x(d)])
    for d in range(1, SIDE):
        left(cf.at[yc], cs_s.at[d])
        left(kp.at[group_of(d) // NZ], ks_s.at[d])
    left(ps.at[1], cs_s.at[0])

    for t in range(T - len(COMBINED)):
        for d in (1, 2, 3):
            left(zs.at[t, at_z(d)], zs_s.at[t, d])

    @pl.when(end)
    def _():
        for t in COMBINED:
            left(zs.at[t, pl.ds(jnp.where(z == 0, 2, 0), 2)], zs_s.at[t, 0])
            left(zs.at[t, beyond], zs_s.at[t, 1])

    @pl.when(middle)
    def _():
        for t in COMBINED:
            left(zs.at[t, beyond], zs_s.at[t, 0])
            left(zc.at[t, 0], zs_s.at[t, 1])
            left(zc.at[t, 1], zs_s.at[t, 2])


def on_device(prior, analysis, increment, truncation):
    vmem = pl.BlockSpec(memory_space=pltpu.VMEM)
    hbm = pl.BlockSpec(memory_space=pltpu.HBM)
    dma = pltpu.SemaphoreType.DMA
    return pl.pallas_call(
        kernel,
        out_shape=pltpu.VMEM((1, LEV, ROWS, NLON), F32),
        in_specs=[hbm, hbm, hbm, hbm],
        out_specs=vmem,
        scratch_shapes=[
            pltpu.VMEM((LEV, ROWS, NLON), BF16),
            pltpu.VMEM((LEV, ROWS, NLON), BF16),
            pltpu.VMEM((ROWS, NLON), F32),
            pltpu.SMEM((LEV,), jnp.int32),
            pltpu.VMEM((NX, T, 2, R, WIDTH), F32),
            pltpu.VMEM((NX, T, 2, R, WIDTH), F32),
            pltpu.VMEM((T, NZ, 4, R, PIECE), F32),
            pltpu.VMEM((T, NZ, 4, R, PIECE), F32),
            pltpu.VMEM((T, 2, 4, R, PIECE), F32),
            pltpu.VMEM((T, NZ, 2, R, PIECE), F32),
            pltpu.VMEM((NX, T, R, WIDTH), F32),
            pltpu.VMEM((SIDE, ROWS, COLS), F32),
            pltpu.VMEM((2, ROWS, COLS), F32),
            pltpu.VMEM((ROWS, COLS), F32),
            pltpu.VMEM((2, QUARTER, COLS), F32),
            pltpu.VMEM((GROUPS, QUARTER, COLS), F32),
            pltpu.VMEM((NLON, COLS), BF16),
            pltpu.VMEM((NLON, COLS), BF16),
            pltpu.VMEM((KEEP, SIDE * ROWS), BF16),
            pltpu.VMEM((KEEP, SIDE * ROWS), BF16),
            pltpu.VMEM((GROUPS * COLS, HALF), BF16),
            pltpu.VMEM((GROUPS * COLS, HALF), BF16),
            pltpu.VMEM((QUARTER, NLON), F32),
            dma((T, NX)), dma((T, NX)),
            dma((T, NZ)), dma((T, NZ)),
            dma((T, NZ)), dma((T, NZ)),
            dma((T, NX)), dma((T, NX)),
            dma((SIDE,)), dma((SIDE + 1,)),
            dma((GROUPS,)), dma((GROUPS,)),
            dma((4,)), pltpu.SemaphoreType.REGULAR((4,)),
        ],
        compiler_params=pltpu.CompilerParams(collective_id=0, has_side_effects=True),
    )(prior, analysis, increment, truncation).astype(BF16)


def solution(mesh):
    placed = (
        P("member", None, "band", None),
        P("member", None, "band", None),
        P(None, "band", None),
        P(),
    )
    return jax.shard_map(
        on_device,
        mesh=mesh,
        in_specs=placed,
        out_specs=P("member", None, "band", None),
        check_vma=False,
    )
```
